32 devices in a mesh: groups: 1, rank: 32 (over z, y, x, core).
Axes of the slice: x: 2, y: 2, z: 4, core: 2. Of those that a mesh axis runs over, the one named last changes fastest.
Arguments:
- core: float32 [256, 256, 256], P('rank', 'groups'), may hold values from -6 to 6
- x_factor: float32 [1536, 256], P('groups'), may hold values from -0.375 to 0.375
- y_factor: float32 [2048, 256], P('groups'), may hold values from -0.375 to 0.375
- z_factor: float32 [256, 1536], P('rank', 'groups'), may hold values from -0.375 to 0.375
- offsets: int32 [8], P('groups'), may hold values from 0 to 1535, as said below
- initial: float32 [1536, 8, 2048], P('rank', 'groups'), may hold values from -80 to 80
Outputs:
- max_error: float32 [1], P('groups')
- psnr: float32 [8], P('groups')
- ssim_five: float32 [1536, 8, 2048], P('rank', 'groups')
- ssim_seven: float32 [1536, 8, 2048], P('rank', 'groups')
- ssim_eleven: float32 [1536, 8, 2048], P('rank', 'groups')
The draws below stay inside these ranges and needn't reach their ends.
Inputs may be any that keep to these rules, and one draw needn't show every extreme that they name: `offsets`: 8 distinct planes in increasing order.
All inputs are finite; a program needn't handle non-finite values.
Results may differ from the reference program's by a relative error of at most 0.000075.
Values sent between devices are 32-bit elements; how exact they have to be, the bound alone decides.
No kernel may reach another device: no remote copies, remote signals or barrier semaphores. Data moves between devices by JAX's collectives and lax.ppermute only.
A program may use at most 128 MiB of HBM per device.

```python
import jax
import jax.numpy as jnp
from jax import lax

R = 256
NX = 1536
NY = 2048
NZ = 1536
PLANES = 8


def draw_initial(key, part):
    keys = jax.random.split(jax.random.fold_in(key, 11), 3)
    positions = jnp.arange(NX, dtype=jnp.float32) / float(NX)
    base = jnp.clip(jax.random.normal(keys[0], (NX, PLANES, NY), jnp.float32), -5.0, 5.0)
    rising = jnp.exp(positions * jnp.log(4.0))
    row_scale = rising * jnp.exp(jax.random.uniform(keys[1], (NX,), jnp.float32, -0.35, 0.35))
    column_scale = jnp.exp(jax.random.uniform(keys[2], (NY,), jnp.float32, -0.7, 0.7))
    return base * row_scale[:, None, None] * column_scale[None, None, :]


def draw_offsets(key, part):
    shuffled = jax.random.permutation(jax.random.fold_in(key, 23), NZ)
    return jnp.sort(shuffled[:PLANES]).astype(jnp.int32)


def steps_of(key, dims, pieces, low, top_value):
    gain, own = 1.0, jax.random.fold_in(key, 6)
    for dim, shards_of in pieces:
        heights = jnp.exp(jax.random.uniform(jax.random.fold_in(own, dim), (shards_of,), jnp.float32, low / len(pieces), top_value / len(pieces)))
        gain = gain * jnp.repeat(heights, dims[dim] // shards_of).reshape([-1 if axis == dim else 1 for axis in range(len(dims))])
    return gain


def noise(own_key, dims, scale, reach, pieces=(), kind=jnp.bfloat16):
    values = scale * jax.random.normal(own_key, dims, jnp.float32)
    if pieces:
        values = values * steps_of(own_key, dims, pieces, -0.22, 0.18)
    return jnp.clip(values, -reach, reach).astype(kind)


def setup_inputs(seed: int = 0, part: int = 0) -> dict:
    key_of = jax.random.split(jax.random.key(seed), 7)
    own_keys = jax.random.split(jax.random.fold_in(key_of[6], part), 7)
    return {
        "core": noise(own_keys[0], (R, R, R), 1.0, 6.0, ((0, 32),), jnp.float32),
        "x_factor": noise(own_keys[1], (NX, R), R ** -0.5, 0.375, (), jnp.float32),
        "y_factor": noise(own_keys[2], (NY, R), R ** -0.5, 0.375, (), jnp.float32),
        "z_factor": noise(own_keys[3], (R, NZ), R ** -0.5, 0.375, ((0, 32),), jnp.float32),
        "offsets": draw_offsets(jax.random.fold_in(jax.random.fold_in(key_of[6], part), 71), part),
        "initial": draw_initial(jax.random.fold_in(jax.random.fold_in(key_of[6], part), 71), part),
    }


peak_value = 64.0
first_const = (0.01 * peak_value) * (0.01 * peak_value)
second_const = (0.03 * peak_value) * (0.03 * peak_value)
epsilon = 1e-6


def box_sums(values, window):
    margin = window // 2
    length = values.shape[0]
    across = values.shape[1]
    padded = jnp.pad(values, ((margin, margin), (0, 0)))
    row_sums = padded[0:length]
    for step_index in range(1, window):
        row_sums = row_sums + padded[step_index:step_index + length]
    padded = jnp.pad(row_sums, ((0, 0), (margin, margin)))
    summed = padded[:, 0:across]
    for step_index in range(1, window):
        summed = summed + padded[:, step_index:step_index + across]
    return summed


def similarity(sum_target, sum_rebuilt, sum_tt, sum_rr, sum_tr, window):
    window_area = float(window * window)
    mean_target = sum_target / window_area
    mean_rebuilt = sum_rebuilt / window_area
    var_target = sum_tt / window_area - mean_target * mean_target
    var_rebuilt = sum_rr / window_area - mean_rebuilt * mean_rebuilt
    covar = sum_tr / window_area - mean_target * mean_rebuilt
    upper = (2.0 * mean_target * mean_rebuilt + first_const) * (2.0 * covar + second_const)
    lower = (mean_target * mean_target + mean_rebuilt * mean_rebuilt + first_const) * (var_target + var_rebuilt + second_const)
    return upper / lower


def plane_maps(pair):
    target_plane, rebuilt_plane = pair
    results = []
    for window in (5, 7, 11):
        results.append(similarity(box_sums(target_plane, window), box_sums(rebuilt_plane, window),
                                  box_sums(target_plane * target_plane, window),
                                  box_sums(rebuilt_plane * rebuilt_plane, window),
                                  box_sums(target_plane * rebuilt_plane, window), window))
    return results[0], results[1], results[2]


def reference(core, x_factor, y_factor, z_factor, offsets, initial):
    exact = lax.Precision.HIGHEST
    picked = jnp.take(z_factor, offsets.astype(jnp.int32), axis=1)
    planes_core = jnp.einsum("kab,kp->pab", core, picked, precision=exact)
    along_y = jnp.einsum("pab,yb->pay", planes_core, y_factor, precision=exact)
    rebuilt = jnp.einsum("xa,pay->xpy", x_factor, along_y, precision=exact)
    misfit = initial - rebuilt
    max_error = jnp.max(jnp.abs(misfit)).reshape(1)
    mean_square = jnp.sum(misfit * misfit, axis=(0, 2)) / float(NX * NY)
    psnr = 10.0 * jnp.log10(peak_value * peak_value / (mean_square + epsilon))
    maps = lax.map(plane_maps, (jnp.moveaxis(initial, 1, 0), jnp.moveaxis(rebuilt, 1, 0)))
    return (max_error, psnr, jnp.moveaxis(maps[0], 0, 1), jnp.moveaxis(maps[1], 0, 1),
            jnp.moveaxis(maps[2], 0, 1))
```

```python
import functools

import jax
import jax.numpy as jnp
from jax import lax
from jax.experimental import pallas as pl
from jax.experimental.pallas import tpu as pltpu
from jax.sharding import PartitionSpec as P

peak_value = 64.0
first_const = 0.01 * peak_value * (0.01 * peak_value)
second_const = 0.03 * peak_value * (0.03 * peak_value)
epsilon = 1e-06
reach = 5
edge = 8
lanes = 128
exact = lax.Precision.HIGHEST
windows = (5, 7, 11)


def vmem(limit=60):
    return pltpu.CompilerParams(vmem_limit_bytes=limit * 1024 * 1024)


def slab_sums(core, z_factor, offsets, me, slots):
    depth, rows, across = core.shape
    block = rows // 4
    count = len(slots)

    def kernel(off, who, *refs):
        z_refs, core_ref, out, scale = refs[:count], refs[count], refs[count + 1], refs[count + 2]

        @pl.when(pl.program_id(0) == 0)
        def _():
            lane = lax.broadcasted_iota(jnp.int32, (depth, lanes), 1)
            for index, slot in enumerate(slots):
                at = off[who[0] ^ slot] % lanes
                column = jnp.sum(
                    jnp.where(lane == at, z_refs[index][...], 0.0), axis=1, keepdims=True
                )
                for k in range(depth):
                    scale[index, k] = jnp.broadcast_to(column[k : k + 1], (8, lanes))

        def step(t, _):
            base = pl.multiple_of(t * 16, 16)
            tiles = [(r, c) for r in range(2) for c in range(across // lanes)]
            held = [
                [
                    core_ref[k, pl.ds(base + 8 * r, 8), c * lanes : (c + 1) * lanes]
                    for r, c in tiles
                ]
                for k in range(depth)
            ]
            for index in range(count):
                sums = [None] * len(tiles)
                for k in range(depth):
                    weight = scale[index, k]
                    for i in range(len(tiles)):
                        term = held[k][i] * weight
                        sums[i] = term if sums[i] is None else sums[i] + term
                for i, (r, c) in enumerate(tiles):
                    out[index, pl.ds(base + 8 * r, 8), c * lanes : (c + 1) * lanes] = sums[i]
            return 0

        lax.fori_loop(0, block // 16, step, 0)

    def z_spec(slot):
        return pl.BlockSpec((depth, lanes), lambda i, off, who: (0, off[who[0] ^ slot] // lanes))

    return pl.pallas_call(
        kernel,
        out_shape=jax.ShapeDtypeStruct((count, rows, across), jnp.float32),
        grid_spec=pltpu.PrefetchScalarGridSpec(
            num_scalar_prefetch=2,
            grid=(4,),
            in_specs=[z_spec(s) for s in slots]
            + [pl.BlockSpec((depth, block, across), lambda i, off, who: (0, i, 0))],
            out_specs=pl.BlockSpec((count, block, across), lambda i, off, who: (0, i, 0)),
            scratch_shapes=[pltpu.VMEM((count, depth, 8, lanes), jnp.float32)],
        ),
        compiler_params=vmem(),
        cost_estimate=pl.CostEstimate(
            flops=2 * count * depth * rows * across, bytes_accessed=8 * rows * across * 4, transcendentals=0
        ),
        name="slab_sums",
    )(offsets, me, *([z_factor] * count), core)


def pair_sums(kept, came):
    count = kept.shape[0]

    def kernel(a, b, *outs):
        for i in range(count):
            outs[i][...] = a[i] + b[i]

    return pl.pallas_call(
        kernel,
        out_shape=[jax.ShapeDtypeStruct(kept.shape[1:], jnp.float32)] * count,
        compiler_params=vmem(),
        name="pair_sums",
    )(kept, came)


def split_sums(parts, layer, layers):
    rows, across = parts[0].shape
    chunk = rows // layers

    def kernel(at, *refs):
        ins, outs = refs[: len(parts)], refs[len(parts) :]
        for m in range(layers):
            start = pl.multiple_of((at[0] ^ m) * chunk, chunk)
            total = ins[0][pl.ds(start, chunk), :]
            for other in ins[1:]:
                total = total + other[pl.ds(start, chunk), :]
            outs[m][...] = total

    return pl.pallas_call(
        kernel,
        out_shape=[jax.ShapeDtypeStruct((chunk, across), jnp.float32)] * layers,
        in_specs=[pl.BlockSpec(memory_space=pltpu.SMEM)]
        + [pl.BlockSpec(memory_space=pltpu.VMEM)] * len(parts),
        compiler_params=vmem(),
        name="split_sums",
    )(layer, *parts)


def sum_all(parts):
    def kernel(*refs):
        total = refs[0][...]
        for other in refs[1:-1]:
            total = total + other[...]
        refs[-1][...] = total

    return pl.pallas_call(
        kernel,
        out_shape=jax.ShapeDtypeStruct(parts[0].shape, jnp.float32),
        compiler_params=vmem(),
        name="sum_all",
    )(*parts)


def expand_rows(chunks, layer, x_rows, planes, rows):
    layers = len(chunks)
    chunk, across = chunks[0].shape

    def kernel(at, *refs):
        pieces, x_ref, out, whole, product = refs[:layers], *refs[layers:]
        for m in range(layers):
            whole[pl.ds(pl.multiple_of((at[0] ^ m) * chunk, chunk), chunk), :] = pieces[m][...]
        product[...] = jnp.dot(
            x_ref[...], whole[...], precision=exact, preferred_element_type=jnp.float32
        )
        for q in range(planes):
            out[q] = product[q * rows : q * rows + rows + 2 * edge, :]

    return pl.pallas_call(
        kernel,
        out_shape=jax.ShapeDtypeStruct((planes, rows + 2 * edge, across), jnp.float32),
        in_specs=[pl.BlockSpec(memory_space=pltpu.SMEM)]
        + [pl.BlockSpec(memory_space=pltpu.VMEM)] * (layers + 1),
        scratch_shapes=[
            pltpu.VMEM((layers * chunk, across), jnp.float32),
            pltpu.VMEM((x_rows.shape[0], across), jnp.float32),
        ],
        compiler_params=vmem(),
        name="expand_rows",
    )(layer, *chunks, x_rows)


def rebuild(block, y_factor, initial):
    planes, tall, depth = block.shape
    rows = tall - 2 * edge
    across = y_factor.shape[0]
    wide = 512
    steps = across // wide
    held = rows + 2 * reach

    def kernel(block_ref, y_ref, init_ref, out, stats, left):
        step = pl.program_id(0)

        @pl.when(step == 0)
        def _():
            for p in range(planes):
                left[:, p, :] = block_ref[p, edge - reach : edge + rows + reach, :]
            zeros = jnp.zeros((held, planes, lanes), jnp.float32)
            out[:, :, :lanes] = zeros
            out[:, :, across + lanes :] = zeros
            stats[...] = jnp.zeros(stats.shape, jnp.float32)

        value = lax.dot_general(
            left[...].reshape(held * planes, depth),
            y_ref[...],
            (((1,), (1,)), ((), ())),
            precision=exact,
            preferred_element_type=jnp.float32,
        ).reshape(held, planes, wide)
        start = pl.multiple_of(lanes + step * wide, lanes)
        out[:, :, pl.ds(start, wide)] = value
        square = jnp.zeros((planes, lanes), jnp.float32)
        top = jnp.zeros((planes, lanes), jnp.float32)
        misfit = init_ref[...] - value[reach : reach + rows]
        squares = jnp.sum(misfit * misfit, axis=0)
        tops = jnp.max(jnp.abs(misfit), axis=0)
        for c in range(wide // lanes):
            square = square + squares[:, c * lanes : (c + 1) * lanes]
            top = jnp.maximum(top, tops[:, c * lanes : (c + 1) * lanes])
        stats[0] += square
        stats[1] = jnp.maximum(stats[1], top)

    return pl.pallas_call(
        kernel,
        grid=(steps,),
        out_shape=[
            jax.ShapeDtypeStruct((held, planes, across + 2 * lanes), jnp.float32),
            jax.ShapeDtypeStruct((2, planes, lanes), jnp.float32),
        ],
        in_specs=[
            pl.BlockSpec(block.shape, lambda i: (0, 0, 0)),
            pl.BlockSpec((wide, depth), lambda i: (i, 0)),
            pl.BlockSpec((rows, planes, wide), lambda i: (0, 0, i)),
        ],
        out_specs=[
            pl.BlockSpec((held, planes, across + 2 * lanes), lambda i: (0, 0, 0)),
            pl.BlockSpec((2, planes, lanes), lambda i: (0, 0, 0)),
        ],
        scratch_shapes=[pltpu.VMEM((held, planes, depth), jnp.float32)],
        compiler_params=vmem(),
        name="rebuild",
    )(block, y_factor, initial)


def across_sums(field, wide):
    total = field.shape[-1]

    def moved(value, by):
        return pltpu.roll(value, (-by) % total, axis=1)

    pair = field + moved(field, 1)
    five = pair + moved(pair, -2) + moved(field, 2)
    seven = five + moved(field, -3) + moved(field, 3)
    eleven = seven + moved(pair, -5) + moved(pair, 4)
    return [value[:, lanes : lanes + wide] for value in (five, seven, eleven)]


def down_sums(load, window, count):
    rows = [load(i) for i in range(count + window - 1)]
    pair = [rows[i] + rows[i + 1] for i in range(count + window - 2)]
    if window == 5:
        return [(pair[i] + pair[i + 2]) + rows[i + 4] for i in range(count)]
    if window == 7:
        return [(pair[i] + pair[i + 2]) + (pair[i + 4] + rows[i + 6]) for i in range(count)]
    four = [pair[i] + pair[i + 2] for i in range(count + 4)]
    return [(four[i] + four[i + 4]) + (pair[i + 8] + rows[i + 10]) for i in range(count)]


def similarity(s1, s2, sq, sx, window):
    area = float(window * window)
    cross = s1 * s2
    twice = cross + cross
    squares = s1 * s1 + s2 * s2
    upper = (twice + area * area * first_const) * (
        (2.0 * area) * sx - twice + area * area * second_const
    )
    lower = (squares + area * area * first_const) * (
        area * sq - squares + area * area * second_const
    )
    return upper / lower


def maps(initial, low, high, rebuilt):
    rows, planes, across = initial.shape
    held = rows + 2 * reach
    wide = 512
    steps = across // wide
    group = 4

    def kernel(init_ref, low_ref, high_ref, reb_ref, out5, out7, out11, ext, sums):
        step = pl.program_id(0)

        @pl.when(step == 0)
        def _():
            zeros = jnp.zeros((held, planes, lanes), jnp.float32)
            ext[:, :, :lanes] = zeros
            ext[:, :, across + lanes :] = zeros
            ext[0:reach, :, lanes : across + lanes] = low_ref[...]
            ext[reach : reach + rows, :, lanes : across + lanes] = init_ref[...]
            ext[reach + rows :, :, lanes : across + lanes] = high_ref[...]

        start = pl.multiple_of(step * wide, lanes)

        def row_step(x, _):
            a = ext[x, :, pl.ds(start, wide + 2 * lanes)]
            b = reb_ref[x, :, pl.ds(start, wide + 2 * lanes)]
            for f, field in enumerate((a, b, a * a + b * b, a * b)):
                for w, value in enumerate(across_sums(field, wide)):
                    sums[f, w, x] = value
            return 0

        lax.fori_loop(0, held, row_step, 0)

        def out_step(t, _):
            base = t * group
            for c in range(wide // lanes):
                part = slice(c * lanes, (c + 1) * lanes)
                for w, (window, out) in enumerate(zip(windows, (out5, out7, out11))):
                    skip = reach - window // 2
                    found = [
                        down_sums(
                            lambda i, f=f: sums[f, w, base + skip + i, :, part], window, group
                        )
                        for f in range(4)
                    ]
                    for i in range(group):
                        out[base + i, :, part] = similarity(
                            found[0][i], found[1][i], found[2][i], found[3][i], window
                        )
            return 0

        lax.fori_loop(0, rows // group, out_step, 0)

    whole = pl.BlockSpec((rows, planes, across), lambda i: (0, 0, 0))
    some = pl.BlockSpec((reach, planes, across), lambda i: (0, 0, 0))
    out_spec = pl.BlockSpec((rows, planes, wide), lambda i: (0, 0, i))
    return pl.pallas_call(
        kernel,
        grid=(steps,),
        out_shape=[jax.ShapeDtypeStruct((rows, planes, across), jnp.float32)] * 3,
        in_specs=[
            whole,
            some,
            some,
            pl.BlockSpec((held, planes, across + 2 * lanes), lambda i: (0, 0, 0)),
        ],
        out_specs=[out_spec] * 3,
        scratch_shapes=[
            pltpu.VMEM((held, planes, across + 2 * lanes), jnp.float32),
            pltpu.VMEM((4, 3, held, planes, wide), jnp.float32),
        ],
        compiler_params=vmem(),
        name="maps",
    )(initial, low, high, rebuilt)


def body(count, core, x_factor, y_factor, z_factor, offsets, initial):
    planes = offsets.shape[0]
    rows = initial.shape[0]
    layers = count // planes
    across = y_factor.shape[0]
    index = lax.axis_index("rank").astype(jnp.int32)
    me = (index % planes).reshape(1)
    layer = (index // planes).reshape(1)

    def swap(value, mask):
        return lax.ppermute(value, "rank", [(i, i ^ mask) for i in range(count)])

    up = [(i, i + 1) for i in range(count - 1)]
    down = [(j, i) for i, j in up]
    low = lax.ppermute(initial[rows - reach :], "rank", up)
    high = lax.ppermute(initial[:reach], "rank", down)

    away = slab_sums(core, z_factor, offsets, me, tuple(range(1, planes, 2)))
    came = swap(away, 1)
    kept = slab_sums(core, z_factor, offsets, me, tuple(range(0, planes, 2)))
    slots = pair_sums(kept, came)
    parts = [slots[0]] + [swap(slots[i], 2 * i) for i in range(1, planes // 2)]
    chunks = split_sums(parts, layer, layers)
    mine = sum_all([chunks[0]] + [swap(chunks[m], planes * m) for m in range(1, layers)])
    pieces = [mine] + [swap(mine, planes * m) for m in range(1, layers)]
    padded = jnp.pad(x_factor, ((edge, edge), (0, 0)))
    x_rows = lax.dynamic_slice_in_dim(
        padded, layer[0] * (planes * rows), planes * rows + 2 * edge, axis=0
    )
    spread = expand_rows(pieces, layer, x_rows, planes, rows)
    groups = [[g * planes + q for q in range(planes)] for g in range(layers)]
    block = lax.all_to_all(
        spread, "rank", split_axis=0, concat_axis=0, tiled=True, axis_index_groups=groups
    )
    rebuilt, stats = rebuild(block, y_factor, initial)
    five, seven, eleven = maps(initial, low, high, rebuilt)
    mask = 1
    while mask < count:
        other = swap(stats, mask)
        stats = jnp.stack((stats[0] + other[0], jnp.maximum(stats[1], other[1])))
        mask *= 2
    max_error = jnp.max(stats[1]).reshape(1)
    mean_square = jnp.sum(stats[0], axis=1) / float(x_factor.shape[0] * across)
    psnr = 10.0 * jnp.log10(peak_value * peak_value / (mean_square + epsilon))
    return max_error, psnr, five, seven, eleven


def solution(mesh):
    placed = (
        P("rank", "groups", None),
        P("groups", None),
        P("groups", None),
        P("rank", "groups"),
        P("groups"),
        P("rank", "groups", None),
    )
    return jax.shard_map(
        functools.partial(body, mesh.shape["rank"]),
        mesh=mesh,
        in_specs=placed,
        out_specs=(
            P("groups"),
            P("groups"),
            P("rank", "groups", None),
            P("rank", "groups", None),
            P("rank", "groups", None),
        ),
        check_vma=False,
    )
```

```python
import functools

import jax
import jax.numpy as jnp
from jax import lax
from jax.experimental import pallas as pl
from jax.experimental.pallas import tpu as pltpu
from jax.sharding import PartitionSpec as P

peak_value = 64.0
first_const = 0.01 * peak_value * (0.01 * peak_value)
second_const = 0.03 * peak_value * (0.03 * peak_value)
epsilon = 1e-06
reach = 5
edge = 8
lanes = 128
exact = lax.Precision.HIGHEST
windows = (5, 7, 11)


def vmem(limit=60):
    return pltpu.CompilerParams(vmem_limit_bytes=limit * 1024 * 1024)


def cost(seconds):
    return pl.CostEstimate(flops=int(seconds * 2e12), bytes_accessed=0, transcendentals=0)


def slab_sums(core, z_factor, offsets, me, slots, came=None):
    depth, rows, across = core.shape
    steps = 2
    block = rows // steps
    count = len(slots)

    def kernel(off, who, *refs):
        z_refs, core_ref, scale = refs[:count], refs[count], refs[-1]
        outs = refs[count + 1 : -1]
        if came is not None:
            came_ref, outs = outs[0], outs[1:]

        @pl.when(pl.program_id(0) == 0)
        def _():
            lane = lax.broadcasted_iota(jnp.int32, (depth, lanes), 1)
            for index, slot in enumerate(slots):
                at = off[who[0] ^ slot] % lanes
                column = jnp.sum(
                    jnp.where(lane == at, z_refs[index][...], 0.0), axis=1, keepdims=True
                )
                for k in range(depth):
                    scale[index, k] = jnp.broadcast_to(column[k : k + 1], (8, lanes))

        def step(t, _):
            base = pl.multiple_of(t * 16, 16)
            tiles = [
                (pl.ds(base + 8 * r, 8), slice(c * lanes, (c + 1) * lanes))
                for r in range(2)
                for c in range(across // lanes)
            ]
            held = [[core_ref[k, r, c] for r, c in tiles] for k in range(depth)]
            for index in range(count):
                if came is None:
                    sums = [None] * len(tiles)
                else:
                    sums = [came_ref[index, r, c] for r, c in tiles]
                for k in range(depth):
                    weight = scale[index, k]
                    for i in range(len(tiles)):
                        term = held[k][i] * weight
                        sums[i] = term if sums[i] is None else sums[i] + term
                for i, (r, c) in enumerate(tiles):
                    if came is None:
                        outs[0][index, r, c] = sums[i]
                    else:
                        outs[index][r, c] = sums[i]
            return 0

        lax.fori_loop(0, block // 16, step, 0)

    def z_spec(slot):
        return pl.BlockSpec((depth, lanes), lambda i, off, who: (0, off[who[0] ^ slot] // lanes))

    stack_spec = pl.BlockSpec((count, block, across), lambda i, off, who: (0, i, 0))
    if came is None:
        out_shape = jax.ShapeDtypeStruct((count, rows, across), jnp.float32)
        out_specs = stack_spec
    else:
        out_shape = [jax.ShapeDtypeStruct((rows, across), jnp.float32)] * count
        out_specs = [pl.BlockSpec((block, across), lambda i, off, who: (i, 0))] * count
    return pl.pallas_call(
        kernel,
        out_shape=out_shape,
        grid_spec=pltpu.PrefetchScalarGridSpec(
            num_scalar_prefetch=2,
            grid=(steps,),
            in_specs=[z_spec(s) for s in slots]
            + [pl.BlockSpec((depth, block, across), lambda i, off, who: (0, i, 0))]
            + ([] if came is None else [stack_spec]),
            out_specs=out_specs,
            scratch_shapes=[pltpu.VMEM((count, depth, 8, lanes), jnp.float32)],
        ),
        compiler_params=vmem(),
        cost_estimate=cost(2e-6),
        name="slab_sums",
    )(offsets, me, *([z_factor] * count), core, *(() if came is None else (came,)))


def split_sums(parts, layer, layers, token):
    rows, across = parts[0].shape
    chunk = rows // layers

    def kernel(at, *refs):
        ins, outs = refs[: len(parts)], refs[len(parts) + 1 :]
        for m in range(layers):
            start = pl.multiple_of((at[0] ^ m) * chunk, chunk)
            total = ins[0][pl.ds(start, chunk), :]
            for other in ins[1:]:
                total = total + other[pl.ds(start, chunk), :]
            outs[m][...] = total

    return pl.pallas_call(
        kernel,
        out_shape=[jax.ShapeDtypeStruct((chunk, across), jnp.float32)] * layers,
        in_specs=[pl.BlockSpec(memory_space=pltpu.SMEM)]
        + [pl.BlockSpec(memory_space=pltpu.VMEM)] * len(parts)
        + [pl.BlockSpec(memory_space=pl.ANY)],
        compiler_params=vmem(),
        name="split_sums",
    )(layer, *parts, token)


def expand_rows(chunks, layer, x_rows, planes, rows):
    layers = len(chunks)
    chunk, across = chunks[0].shape

    def kernel(at, *refs):
        pieces, x_ref, out, whole, product = refs[:layers], *refs[layers:]
        for m in range(layers):
            whole[pl.ds(pl.multiple_of((at[0] ^ m) * chunk, chunk), chunk), :] = pieces[m][...]
        product[...] = jnp.dot(
            x_ref[...], whole[...], precision=exact, preferred_element_type=jnp.float32
        )
        for q in range(planes):
            out[q] = product[q * rows : q * rows + rows + 2 * edge, :]

    return pl.pallas_call(
        kernel,
        out_shape=jax.ShapeDtypeStruct((planes, rows + 2 * edge, across), jnp.float32),
        in_specs=[pl.BlockSpec(memory_space=pltpu.SMEM)]
        + [pl.BlockSpec(memory_space=pltpu.VMEM)] * (layers + 1),
        scratch_shapes=[
            pltpu.VMEM((layers * chunk, across), jnp.float32),
            pltpu.VMEM((x_rows.shape[0], across), jnp.float32),
        ],
        compiler_params=vmem(),
        name="expand_rows",
    )(layer, *chunks, x_rows)


def held_rows(rows):
    return -(-(rows + 2 * reach) // 4) * 4


def rebuild(block, y_padded, extended):
    planes, tall, depth = block.shape
    rows = tall - 2 * edge
    steps = 3
    wide = y_padded.shape[0] // steps
    held = held_rows(rows)

    def kernel(block_ref, y_ref, ext_ref, out, stats, left):
        @pl.when(pl.program_id(0) == 0)
        def _():
            for p in range(planes):
                left[:, p, :] = block_ref[p, edge - reach : edge - reach + held, :]
            stats[...] = jnp.zeros(stats.shape, jnp.float32)

        value = lax.dot_general(
            left[...].reshape(held * planes, depth),
            y_ref[...],
            (((1,), (1,)), ((), ())),
            precision=exact,
            preferred_element_type=jnp.float32,
        ).reshape(held, planes, wide)
        out[...] = value
        misfit = ext_ref[reach : reach + rows] - value[reach : reach + rows]
        squares = jnp.sum(misfit * misfit, axis=0)
        tops = jnp.max(jnp.abs(misfit), axis=0)
        square, top = stats[0], stats[1]
        for c in range(wide // lanes):
            square = square + squares[:, c * lanes : (c + 1) * lanes]
            top = jnp.maximum(top, tops[:, c * lanes : (c + 1) * lanes])
        stats[0] = square
        stats[1] = top

    strip = pl.BlockSpec((held, planes, wide), lambda i: (0, 0, i))
    return pl.pallas_call(
        kernel,
        grid=(steps,),
        out_shape=[
            jax.ShapeDtypeStruct(extended.shape, jnp.float32),
            jax.ShapeDtypeStruct((2, planes, lanes), jnp.float32),
        ],
        in_specs=[
            pl.BlockSpec(block.shape, lambda i: (0, 0, 0)),
            pl.BlockSpec((wide, depth), lambda i: (i, 0)),
            strip,
        ],
        out_specs=[strip, pl.BlockSpec((2, planes, lanes), lambda i: (0, 0, 0))],
        scratch_shapes=[pltpu.VMEM((held, planes, depth), jnp.float32)],
        compiler_params=vmem(),
        cost_estimate=cost(6e-6),
        name="rebuild",
    )(block, y_padded, extended)


def across_sums(field, wide):
    total = field.shape[-1]

    def moved(value, by):
        return pltpu.roll(value, (-by) % total, axis=1)

    pair = field + moved(field, 1)
    five = pair + moved(pair, -2) + moved(field, 2)
    seven = five + moved(field, -3) + moved(field, 3)
    eleven = seven + moved(pair, -5) + moved(pair, 4)
    return [value[:, lanes : lanes + wide] for value in (five, seven, eleven)]


def down_sums(load, window, count):
    rows = [load(i) for i in range(count + window - 1)]
    pair = [rows[i] + rows[i + 1] for i in range(count + window - 2)]
    if window == 5:
        return [(pair[i] + pair[i + 2]) + rows[i + 4] for i in range(count)]
    if window == 7:
        return [(pair[i] + pair[i + 2]) + (pair[i + 4] + rows[i + 6]) for i in range(count)]
    four = [pair[i] + pair[i + 2] for i in range(count + 4)]
    return [(four[i] + four[i + 4]) + (pair[i + 8] + rows[i + 10]) for i in range(count)]


def row_sums(fields, sums, held, wide):
    def step(t, _):
        for j in range(4):
            x = t * 4 + j
            for f, field in enumerate(fields(x)):
                for w, value in enumerate(across_sums(field, wide)):
                    for c in range(wide // lanes):
                        sums[f, w, c, x] = value[:, c * lanes : (c + 1) * lanes]
        return 0

    lax.fori_loop(0, held // 4, step, 0)


def target_sums(initial, low, high, gate):
    rows, planes, across = initial.shape
    held = held_rows(rows)
    wide = 512
    steps = across // wide
    padded = across + 2 * lanes
    group = 8 if rows % 8 == 0 else 4

    def kernel(init_ref, low_ref, high_ref, gate_ref, ext, token, *refs):
        outs, sums = refs[:6], refs[6]
        step = pl.program_id(0)

        @pl.when(step == 0)
        def _():
            token[...] = jnp.zeros(token.shape, jnp.float32)
            zeros = jnp.zeros((held, planes, lanes), jnp.float32)
            ext[:, :, :lanes] = zeros
            ext[:, :, across + lanes :] = zeros
            ext[0:reach, :, lanes : across + lanes] = low_ref[...]
            ext[reach : reach + rows, :, lanes : across + lanes] = init_ref[...]
            ext[reach + rows : rows + 2 * reach, :, lanes : across + lanes] = high_ref[...]
            if held > rows + 2 * reach:
                rest = held - rows - 2 * reach
                ext[rows + 2 * reach :, :, lanes : across + lanes] = jnp.zeros(
                    (rest, planes, across), jnp.float32
                )

        start = pl.multiple_of(step * wide, lanes)
        row_sums(lambda x: (ext[x, :, pl.ds(start, wide + 2 * lanes)],), sums, held, wide)

        def out_step(t, _):
            base = t * group
            for c in range(wide // lanes):
                part = slice(c * lanes, (c + 1) * lanes)
                for w, window in enumerate(windows):
                    area = float(window * window)
                    skip = reach - window // 2
                    found = down_sums(lambda i: sums[0, w, c, base + skip + i], window, group)
                    for i in range(group):
                        double = found[i] * (2.0 / area)
                        outs[2 * w][base + i, :, part] = double
                        outs[2 * w + 1][base + i, :, part] = (
                            double * double * (0.25 * area) + area * first_const
                        )
            return 0

        lax.fori_loop(0, rows // group, out_step, 0)

    some = pl.BlockSpec((reach, planes, across), lambda i: (0, 0, 0))
    out_spec = pl.BlockSpec((rows, planes, wide), lambda i: (0, 0, i))
    return pl.pallas_call(
        kernel,
        grid=(steps,),
        out_shape=[
            jax.ShapeDtypeStruct((held, planes, padded), jnp.float32),
            jax.ShapeDtypeStruct((8, lanes), jnp.float32),
        ]
        + [jax.ShapeDtypeStruct((rows, planes, across), jnp.float32)] * 6,
        in_specs=[
            pl.BlockSpec((rows, planes, across), lambda i: (0, 0, 0)),
            some,
            some,
            pl.BlockSpec(memory_space=pl.ANY),
        ],
        out_specs=[
            pl.BlockSpec((held, planes, padded), lambda i: (0, 0, 0)),
            pl.BlockSpec((8, lanes), lambda i: (0, 0)),
        ]
        + [out_spec] * 6,
        scratch_shapes=[pltpu.VMEM((1, 3, wide // lanes, held, planes, lanes), jnp.float32)],
        compiler_params=vmem(),
        cost_estimate=cost(12e-6),
        name="target_sums",
    )(initial, low, high, gate)


def maps(extended, rebuilt, target, rows):
    held, planes, padded = extended.shape
    across = padded - 2 * lanes
    wide = 512
    steps = across // wide
    group = 8 if rows % 8 == 0 else 4

    def kernel(ext_ref, reb_ref, *refs):
        target_refs, outs, sums = refs[:6], refs[6:9], refs[9]

        def fields(x):
            a = ext_ref[x]
            b = reb_ref[x]
            product = a * b
            return b, a * a + b * b, product + product

        row_sums(fields, sums, held, wide)

        def out_step(t, _):
            base = t * group
            for c in range(wide // lanes):
                part = slice(c * lanes, (c + 1) * lanes)
                for w, window in enumerate(windows):
                    area = float(window * window)
                    skip = reach - window // 2
                    found = [
                        down_sums(lambda i, f=f: sums[f, w, c, base + skip + i], window, group)
                        for f in range(3)
                    ]
                    for i in range(group):
                        one, squares, double = (found[f][i] for f in range(3))
                        twice = target_refs[2 * w][base + i, :, part] * one
                        both = target_refs[2 * w + 1][base + i, :, part] + one * one * (1.0 / area)
                        upper = (twice + area * first_const) * (
                            (double - twice) + area * second_const
                        )
                        lower = both * ((squares - both) + area * (first_const + second_const))
                        outs[w][base + i, :, part] = upper / lower
            return 0

        lax.fori_loop(0, rows // group, out_step, 0)

    out_spec = pl.BlockSpec((rows, planes, wide), lambda i: (0, 0, i))
    strip = pl.BlockSpec(
        (pl.Element(held), pl.Element(planes), pl.Element(wide + 2 * lanes)),
        lambda i: (0, 0, pl.multiple_of(i * wide, lanes)),
    )
    return pl.pallas_call(
        kernel,
        grid=(steps,),
        out_shape=[jax.ShapeDtypeStruct((rows, planes, across), jnp.float32)] * 3,
        in_specs=[strip, strip] + [out_spec] * 6,
        out_specs=[out_spec] * 3,
        scratch_shapes=[pltpu.VMEM((3, 3, wide // lanes, held, planes, lanes), jnp.float32)],
        compiler_params=vmem(),
        cost_estimate=cost(25e-6),
        name="maps",
    )(extended, rebuilt, *target)


def body(count, core, x_factor, y_factor, z_factor, offsets, initial):
    planes = offsets.shape[0]
    rows = initial.shape[0]
    layers = count // planes
    across = y_factor.shape[0]
    index = lax.axis_index("rank").astype(jnp.int32)
    me = (index % planes).reshape(1)
    layer = (index // planes).reshape(1)

    def swap(value, mask):
        return lax.ppermute(value, "rank", [(i, i ^ mask) for i in range(count)])

    up = [(i, i + 1) for i in range(count - 1)]
    down = [(j, i) for i, j in up]
    low = lax.ppermute(initial[rows - reach :], "rank", up)
    high = lax.ppermute(initial[:reach], "rank", down)

    away = slab_sums(core, z_factor, offsets, me, tuple(range(1, planes, 2)))
    came = swap(away, 1)
    slots = slab_sums(core, z_factor, offsets, me, tuple(range(0, planes, 2)), came)
    parts = [slots[0]] + [swap(slots[i], 2 * i) for i in range(1, planes // 2)]
    extended, token, *target = target_sums(initial, low, high, slots[0])
    chunks = split_sums(parts, layer, layers, token)
    mine = chunks[0]
    for m in range(1, layers):
        mine = mine + swap(chunks[m], planes * m)
    pieces = [mine] + [swap(mine, planes * m) for m in range(1, layers)]
    padded = jnp.pad(x_factor, ((edge, edge), (0, 0)))
    x_rows = lax.dynamic_slice_in_dim(
        padded, layer[0] * (planes * rows), planes * rows + 2 * edge, axis=0
    )
    spread = expand_rows(pieces, layer, x_rows, planes, rows)
    groups = [[g * planes + q for q in range(planes)] for g in range(layers)]
    block = lax.all_to_all(
        spread, "rank", split_axis=0, concat_axis=0, tiled=True, axis_index_groups=groups
    )
    y_padded = jnp.pad(y_factor, ((lanes, lanes), (0, 0)))
    rebuilt, stats = rebuild(block, y_padded, extended)
    five, seven, eleven = maps(extended, rebuilt, target, rows)
    mask = 1
    while mask < count:
        other = swap(stats, mask)
        stats = jnp.stack((stats[0] + other[0], jnp.maximum(stats[1], other[1])))
        mask *= 2
    max_error = jnp.max(stats[1]).reshape(1)
    mean_square = jnp.sum(stats[0], axis=1) / float(x_factor.shape[0] * across)
    psnr = 10.0 * jnp.log10(peak_value * peak_value / (mean_square + epsilon))
    return max_error, psnr, five, seven, eleven


def solution(mesh):
    placed = (
        P("rank", "groups", None),
        P("groups", None),
        P("groups", None),
        P("rank", "groups"),
        P("groups"),
        P("rank", "groups", None),
    )
    return jax.shard_map(
        functools.partial(body, mesh.shape["rank"]),
        mesh=mesh,
        in_specs=placed,
        out_specs=(
            P("groups"),
            P("groups"),
            P("rank", "groups", None),
            P("rank", "groups", None),
            P("rank", "groups", None),
        ),
        check_vma=False,
    )
```

```python
import functools

import jax
import jax.numpy as jnp
from jax import lax
from jax.experimental import pallas as pl
from jax.experimental.pallas import tpu as pltpu
from jax.sharding import PartitionSpec as P

peak_value = 64.0
first_const = 0.01 * peak_value * (0.01 * peak_value)
second_const = 0.03 * peak_value * (0.03 * peak_value)
epsilon = 1e-06
reach = 5
edge = 8
lanes = 128
half = 64
exact = lax.Precision.HIGHEST
windows = (5, 7, 11)


def vmem(limit=60):
    return pltpu.CompilerParams(vmem_limit_bytes=limit * 1024 * 1024)


def cost(seconds):
    return pl.CostEstimate(flops=int(seconds * 2e12), bytes_accessed=0, transcendentals=0)


def slab_sums(core, z_factor, offsets, me, slots, came=None):
    depth, rows, across = core.shape
    steps = 2
    block = rows // steps
    count = len(slots)

    def kernel(off, who, *refs):
        z_refs, core_ref, scale = refs[:count], refs[count], refs[-1]
        outs = refs[count + 1 : -1]
        if came is not None:
            came_ref, outs = outs[0], outs[1:]

        @pl.when(pl.program_id(0) == 0)
        def _():
            lane = lax.broadcasted_iota(jnp.int32, (depth, lanes), 1)
            for index, slot in enumerate(slots):
                at = off[who[0] ^ slot] % lanes
                column = jnp.sum(
                    jnp.where(lane == at, z_refs[index][...], 0.0), axis=1, keepdims=True
                )
                for k in range(depth):
                    scale[index, k] = jnp.broadcast_to(column[k : k + 1], (8, lanes))

        def step(t, _):
            base = pl.multiple_of(t * 16, 16)
            tiles = [
                (pl.ds(base + 8 * r, 8), slice(c * lanes, (c + 1) * lanes))
                for r in range(2)
                for c in range(across // lanes)
            ]
            held = [[core_ref[k, r, c] for r, c in tiles] for k in range(depth)]
            for index in range(count):
                if came is None:
                    sums = [None] * len(tiles)
                else:
                    sums = [came_ref[index, r, c] for r, c in tiles]
                for k in range(depth):
                    weight = scale[index, k]
                    for i in range(len(tiles)):
                        term = held[k][i] * weight
                        sums[i] = term if sums[i] is None else sums[i] + term
                for i, (r, c) in enumerate(tiles):
                    if came is None:
                        outs[0][index, r, c] = sums[i]
                    else:
                        outs[index][r, c] = sums[i]
            return 0

        lax.fori_loop(0, block // 16, step, 0)

    def z_spec(slot):
        return pl.BlockSpec((depth, lanes), lambda i, off, who: (0, off[who[0] ^ slot] // lanes))

    stack_spec = pl.BlockSpec((count, block, across), lambda i, off, who: (0, i, 0))
    if came is None:
        out_shape = jax.ShapeDtypeStruct((count, rows, across), jnp.float32)
        out_specs = stack_spec
    else:
        out_shape = [jax.ShapeDtypeStruct((rows, across), jnp.float32)] * count
        out_specs = [pl.BlockSpec((block, across), lambda i, off, who: (i, 0))] * count
    return pl.pallas_call(
        kernel,
        out_shape=out_shape,
        grid_spec=pltpu.PrefetchScalarGridSpec(
            num_scalar_prefetch=2,
            grid=(steps,),
            in_specs=[z_spec(s) for s in slots]
            + [pl.BlockSpec((depth, block, across), lambda i, off, who: (0, i, 0))]
            + ([] if came is None else [stack_spec]),
            out_specs=out_specs,
            scratch_shapes=[pltpu.VMEM((count, depth, 8, lanes), jnp.float32)],
        ),
        compiler_params=vmem(),
        cost_estimate=cost(2e-6),
        name="slab_sums",
    )(offsets, me, *([z_factor] * count), core, *(() if came is None else (came,)))


def split_sums(parts, layer, layers, token):
    rows, across = parts[0].shape
    chunk = rows // layers

    def kernel(at, *refs):
        ins, outs = refs[: len(parts)], refs[len(parts) + 1 :]
        for m in range(layers):
            start = pl.multiple_of((at[0] ^ m) * chunk, chunk)
            total = ins[0][pl.ds(start, chunk), :]
            for other in ins[1:]:
                total = total + other[pl.ds(start, chunk), :]
            outs[m][...] = total

    return pl.pallas_call(
        kernel,
        out_shape=[jax.ShapeDtypeStruct((chunk, across), jnp.float32)] * layers,
        in_specs=[pl.BlockSpec(memory_space=pltpu.SMEM)]
        + [pl.BlockSpec(memory_space=pltpu.VMEM)] * len(parts)
        + [pl.BlockSpec(memory_space=pl.ANY)],
        compiler_params=vmem(),
        name="split_sums",
    )(layer, *parts, token)


def expand_rows(chunks, layer, x_rows, planes, rows, gate):
    layers = len(chunks)
    chunk, across = chunks[0].shape

    def kernel(at, *refs):
        pieces, x_ref, _, out, whole, product = refs[:layers], *refs[layers:]
        for m in range(layers):
            whole[pl.ds(pl.multiple_of((at[0] ^ m) * chunk, chunk), chunk), :] = pieces[m][...]
        product[...] = jnp.dot(
            x_ref[...], whole[...], precision=exact, preferred_element_type=jnp.float32
        )
        for q in range(planes):
            out[q] = product[q * rows : q * rows + rows + 2 * edge, :]

    return pl.pallas_call(
        kernel,
        out_shape=jax.ShapeDtypeStruct((planes, rows + 2 * edge, across), jnp.float32),
        in_specs=[pl.BlockSpec(memory_space=pltpu.SMEM)]
        + [pl.BlockSpec(memory_space=pltpu.VMEM)] * (layers + 1)
        + [pl.BlockSpec(memory_space=pl.ANY)],
        scratch_shapes=[
            pltpu.VMEM((layers * chunk, across), jnp.float32),
            pltpu.VMEM((x_rows.shape[0], across), jnp.float32),
        ],
        compiler_params=vmem(),
        name="expand_rows",
    )(layer, *chunks, x_rows, gate)


def held_rows(rows):
    return -(-(rows + 2 * reach) // 4) * 4


def rebuild(block, y_padded, extended):
    planes, tall, depth = block.shape
    rows = tall - 2 * edge
    steps = 3
    wide = y_padded.shape[0] // steps
    held = held_rows(rows)

    def kernel(block_ref, y_ref, ext_ref, out, stats, boxed, left):
        @pl.when(pl.program_id(0) == 0)
        def _():
            for p in range(planes):
                left[:, p, :] = block_ref[p, edge - reach : edge - reach + held, :]
            stats[...] = jnp.zeros(stats.shape, jnp.float32)
            for w, window in enumerate(windows):
                skip = reach - window // 2
                total = left[skip : skip + rows]
                for i in range(1, window):
                    total = total + left[skip + i : skip + i + rows]
                boxed[w] = total

        value = lax.dot_general(
            left[...].reshape(held * planes, depth),
            y_ref[...],
            (((1,), (1,)), ((), ())),
            precision=exact,
            preferred_element_type=jnp.float32,
        ).reshape(held, planes, wide)
        out[...] = value
        misfit = ext_ref[reach : reach + rows] - value[reach : reach + rows]
        squares = jnp.sum(misfit * misfit, axis=0)
        tops = jnp.max(jnp.abs(misfit), axis=0)
        square, top = stats[0], stats[1]
        for c in range(wide // lanes):
            square = square + squares[:, c * lanes : (c + 1) * lanes]
            top = jnp.maximum(top, tops[:, c * lanes : (c + 1) * lanes])
        stats[0] = square
        stats[1] = top

    strip = pl.BlockSpec((held, planes, wide), lambda i: (0, 0, i))
    return pl.pallas_call(
        kernel,
        grid=(steps,),
        out_shape=[
            jax.ShapeDtypeStruct(extended.shape, jnp.float32),
            jax.ShapeDtypeStruct((2, planes, lanes), jnp.float32),
            jax.ShapeDtypeStruct((3, rows, planes, depth), jnp.float32),
        ],
        in_specs=[
            pl.BlockSpec(block.shape, lambda i: (0, 0, 0)),
            pl.BlockSpec((wide, depth), lambda i: (i, 0)),
            strip,
        ],
        out_specs=[
            strip,
            pl.BlockSpec((2, planes, lanes), lambda i: (0, 0, 0)),
            pl.BlockSpec((3, rows, planes, depth), lambda i: (0, 0, 0, 0)),
        ],
        scratch_shapes=[pltpu.VMEM((held, planes, depth), jnp.float32)],
        compiler_params=vmem(),
        cost_estimate=cost(6e-6),
        name="rebuild",
    )(block, y_padded, extended)


def down_sums(load, window, count):
    rows = [load(i) for i in range(count + window - 1)]
    pair = [rows[i] + rows[i + 1] for i in range(count + window - 2)]
    if window == 5:
        return [(pair[i] + pair[i + 2]) + rows[i + 4] for i in range(count)]
    if window == 7:
        return [(pair[i] + pair[i + 2]) + (pair[i + 4] + rows[i + 6]) for i in range(count)]
    four = [pair[i] + pair[i + 2] for i in range(count + 4)]
    return [(four[i] + four[i + 4]) + (pair[i + 8] + rows[i + 10]) for i in range(count)]


def band_matrix():
    source = lax.broadcasted_iota(jnp.int32, (2 * lanes, lanes), 0)
    target = lax.broadcasted_iota(jnp.int32, (2 * lanes, lanes), 1) + half
    apart = jnp.abs(source - target)
    return jnp.concatenate(
        [jnp.where(apart <= window // 2, 1.0, 0.0) for window in windows], axis=1
    ).astype(jnp.bfloat16)


def split_store(value, terms, field, at):
    for t in range(3):
        term = value.astype(jnp.bfloat16)
        terms[field, t, at, :] = term
        if t < 2:
            value = value - term.astype(jnp.float32)


def band_sums(count, terms, sums, wide, held, planes):
    band = band_matrix()
    for f in range(count):
        for c in range(wide // lanes):
            total = None
            for t in range(3):
                found = jnp.dot(
                    terms[f, t, :, c * lanes : c * lanes + 2 * lanes],
                    band,
                    preferred_element_type=jnp.float32,
                )
                total = found if total is None else total + found
            for w in range(3):
                sums[f, w, c] = total[:, w * lanes : (w + 1) * lanes].reshape(held, planes, lanes)


def target_sums(initial, low, high, gate):
    rows, planes, across = initial.shape
    held = held_rows(rows)
    wide = 512
    steps = across // wide
    padded = across + 2 * lanes
    group = 8 if rows % 8 == 0 else 4

    def kernel(init_ref, low_ref, high_ref, gate_ref, ext, token, *refs):
        outs, terms, sums = refs[:6], refs[6], refs[7]
        step = pl.program_id(0)

        @pl.when(step == 0)
        def _():
            token[...] = jnp.zeros(token.shape, jnp.float32)

            def copy_row(ref):
                def go(x, at):
                    ext[at + x, :, 0:lanes] = jnp.zeros((planes, lanes), jnp.float32)
                    ext[at + x, :, across : across + 2 * lanes] = jnp.zeros(
                        (planes, 2 * lanes), jnp.float32
                    )
                    ext[at + x, :, half : half + across] = ref[x]
                    return at

                return go

            lax.fori_loop(0, reach, copy_row(low_ref), 0)
            lax.fori_loop(0, rows, copy_row(init_ref), reach)
            lax.fori_loop(0, reach, copy_row(high_ref), reach + rows)
            for x in range(rows + 2 * reach, held):
                ext[x] = jnp.zeros((planes, padded), jnp.float32)

        start = pl.multiple_of(step * wide, lanes)

        def split_step(t, _):
            value = ext[pl.ds(t * 2, 2), :, pl.ds(start, wide + lanes)]
            at = pl.ds(pl.multiple_of(t * 2 * planes, 2 * planes), 2 * planes)
            split_store(value.reshape(2 * planes, wide + lanes), terms, 0, at)
            return 0

        lax.fori_loop(0, held // 2, split_step, 0)
        band_sums(1, terms, sums, wide, held, planes)

        def out_step(t, _):
            base = t * group
            for c in range(wide // lanes):
                part = slice(c * lanes, (c + 1) * lanes)
                for w, window in enumerate(windows):
                    area = float(window * window)
                    skip = reach - window // 2
                    found = down_sums(lambda i: sums[0, w, c, base + skip + i], window, group)
                    for i in range(group):
                        double = found[i] * (2.0 / window)
                        outs[2 * w][base + i, :, part] = double
                        outs[2 * w + 1][base + i, :, part] = (
                            double * double * 0.25 + area * first_const
                        )
            return 0

        lax.fori_loop(0, rows // group, out_step, 0)

    some = pl.BlockSpec((reach, planes, across), lambda i: (0, 0, 0))
    out_spec = pl.BlockSpec((rows, planes, wide), lambda i: (0, 0, i))
    return pl.pallas_call(
        kernel,
        grid=(steps,),
        out_shape=[
            jax.ShapeDtypeStruct((held, planes, padded), jnp.float32),
            jax.ShapeDtypeStruct((8, lanes), jnp.float32),
        ]
        + [jax.ShapeDtypeStruct((rows, planes, across), jnp.float32)] * 6,
        in_specs=[
            pl.BlockSpec((rows, planes, across), lambda i: (0, 0, 0)),
            some,
            some,
            pl.BlockSpec(memory_space=pl.ANY),
        ],
        out_specs=[
            pl.BlockSpec((held, planes, padded), lambda i: (0, 0, 0)),
            pl.BlockSpec((8, lanes), lambda i: (0, 0)),
        ]
        + [out_spec] * 6,
        scratch_shapes=[
            pltpu.VMEM((1, 3, held * planes, wide + lanes), jnp.bfloat16),
            pltpu.VMEM((1, 3, wide // lanes, held, planes, lanes), jnp.float32),
        ],
        compiler_params=vmem(),
        cost_estimate=cost(12e-6),
        name="target_sums",
    )(initial, low, high, gate)


def maps(extended, rebuilt, boxed, y_boxed, target):
    held, planes, padded = extended.shape
    rows, depth = boxed.shape[1], boxed.shape[3]
    across = padded - 2 * lanes
    wide = 512
    steps = across // wide
    group = 8 if rows % 8 == 0 else 4

    def kernel(ext_ref, reb_ref, boxed_ref, y_ref, *refs):
        target_refs, outs, (terms, sums, plain) = refs[:6], refs[6:9], refs[9:]

        def split_step(t, _):
            a = ext_ref[pl.ds(t * 2, 2)].reshape(2 * planes, wide + lanes)
            b = reb_ref[pl.ds(t * 2, 2)].reshape(2 * planes, wide + lanes)
            product = a * b
            at = pl.ds(pl.multiple_of(t * 2 * planes, 2 * planes), 2 * planes)
            split_store(a * a + b * b, terms, 0, at)
            split_store(product + product, terms, 1, at)
            return 0

        lax.fori_loop(0, held // 2, split_step, 0)
        band_sums(2, terms, sums, wide, held, planes)
        for w, window in enumerate(windows):
            found = lax.dot_general(
                boxed_ref[w].reshape(rows * planes, depth),
                y_ref[w],
                (((1,), (1,)), ((), ())),
                precision=exact,
                preferred_element_type=jnp.float32,
            )
            for c in range(wide // lanes):
                plain[w, c] = found[:, c * lanes : (c + 1) * lanes].reshape(rows, planes, lanes)

        def out_step(t, _):
            base = t * group
            for c in range(wide // lanes):
                part = slice(c * lanes, (c + 1) * lanes)
                for w, window in enumerate(windows):
                    area = float(window * window)
                    skip = reach - window // 2
                    found = [
                        down_sums(lambda i, f=f: sums[f, w, c, base + skip + i], window, group)
                        for f in range(2)
                    ]
                    for i in range(group):
                        squares, double = (found[f][i] for f in range(2))
                        one = plain[w, c, base + i]
                        twice = target_refs[2 * w][base + i, :, part] * one
                        both = target_refs[2 * w + 1][base + i, :, part] + one * one
                        upper = (twice + area * first_const) * (
                            (double - twice) + area * second_const
                        )
                        lower = both * ((squares - both) + area * (first_const + second_const))
                        outs[w][base + i, :, part] = upper / lower
            return 0

        lax.fori_loop(0, rows // group, out_step, 0)

    out_spec = pl.BlockSpec((rows, planes, wide), lambda i: (0, 0, i))
    strip = pl.BlockSpec(
        (pl.Element(held), pl.Element(planes), pl.Element(wide + lanes)),
        lambda i: (0, 0, pl.multiple_of(i * wide, lanes)),
    )
    return pl.pallas_call(
        kernel,
        grid=(steps,),
        out_shape=[jax.ShapeDtypeStruct((rows, planes, across), jnp.float32)] * 3,
        in_specs=[
            strip,
            strip,
            pl.BlockSpec(boxed.shape, lambda i: (0, 0, 0, 0)),
            pl.BlockSpec((3, wide, depth), lambda i: (0, i, 0)),
        ]
        + [out_spec] * 6,
        out_specs=[out_spec] * 3,
        scratch_shapes=[
            pltpu.VMEM((2, 3, held * planes, wide + lanes), jnp.bfloat16),
            pltpu.VMEM((2, 3, wide // lanes, held, planes, lanes), jnp.float32),
            pltpu.VMEM((3, wide // lanes, rows, planes, lanes), jnp.float32),
        ],
        compiler_params=vmem(),
        cost_estimate=cost(25e-6),
        name="maps",
    )(extended, rebuilt, boxed, y_boxed, *target)


def body(count, core, x_factor, y_factor, z_factor, offsets, initial):
    planes = offsets.shape[0]
    rows = initial.shape[0]
    layers = count // planes
    across = y_factor.shape[0]
    index = lax.axis_index("rank").astype(jnp.int32)
    me = (index % planes).reshape(1)
    layer = (index // planes).reshape(1)

    def swap(value, mask):
        return lax.ppermute(value, "rank", [(i, i ^ mask) for i in range(count)])

    up = [(i, i + 1) for i in range(count - 1)]
    down = [(j, i) for i, j in up]
    low = lax.ppermute(initial[rows - reach :], "rank", up)
    high = lax.ppermute(initial[:reach], "rank", down)

    away = slab_sums(core, z_factor, offsets, me, tuple(range(1, planes, 2)))
    came = swap(away, 1)
    slots = slab_sums(core, z_factor, offsets, me, tuple(range(0, planes, 2)), came)
    parts = [slots[0]] + [swap(slots[i], 2 * i) for i in range(1, planes // 2)]
    extended, token, *target = target_sums(initial, low, high, slots[0])
    chunks = split_sums(parts, layer, layers, token)
    mine = chunks[0]
    for m in range(1, layers):
        mine = mine + swap(chunks[m], planes * m)
    pieces = [mine] + [swap(mine, planes * m) for m in range(1, layers)]
    padded = jnp.pad(x_factor, ((edge, edge), (0, 0)))
    x_rows = lax.dynamic_slice_in_dim(
        padded, layer[0] * (planes * rows), planes * rows + 2 * edge, axis=0
    )
    y_padded = jnp.pad(y_factor, ((half, 2 * lanes - half), (0, 0)))
    y_boxed = []
    for window in windows:
        total = y_padded[half - window // 2 :][:across]
        for i in range(1, window):
            total = total + y_padded[half - window // 2 + i :][:across]
        y_boxed.append(total * (1.0 / window))
    y_boxed = jnp.stack(y_boxed)
    spread = expand_rows(pieces, layer, x_rows, planes, rows, y_boxed)
    groups = [[g * planes + q for q in range(planes)] for g in range(layers)]
    block = lax.all_to_all(
        spread, "rank", split_axis=0, concat_axis=0, tiled=True, axis_index_groups=groups
    )
    rebuilt, stats, boxed = rebuild(block, y_padded, extended)
    five, seven, eleven = maps(extended, rebuilt, boxed, y_boxed, target)
    mask = 1
    while mask < count:
        other = swap(stats, mask)
        stats = jnp.stack((stats[0] + other[0], jnp.maximum(stats[1], other[1])))
        mask *= 2
    max_error = jnp.max(stats[1]).reshape(1)
    mean_square = jnp.sum(stats[0], axis=1) / float(x_factor.shape[0] * across)
    psnr = 10.0 * jnp.log10(peak_value * peak_value / (mean_square + epsilon))
    return max_error, psnr, five, seven, eleven


def solution(mesh):
    placed = (
        P("rank", "groups", None),
        P("groups", None),
        P("groups", None),
        P("rank", "groups"),
        P("groups"),
        P("rank", "groups", None),
    )
    return jax.shard_map(
        functools.partial(body, mesh.shape["rank"]),
        mesh=mesh,
        in_specs=placed,
        out_specs=(
            P("groups"),
            P("groups"),
            P("rank", "groups", None),
            P("rank", "groups", None),
            P("rank", "groups", None),
        ),
        check_vma=False,
    )
```

```python
import functools

import jax
import jax.numpy as jnp
from jax import lax
from jax.experimental import pallas as pl
from jax.experimental.pallas import tpu as pltpu
from jax.sharding import PartitionSpec as P

peak_value = 64.0
first_const = 0.01 * peak_value * (0.01 * peak_value)
second_const = 0.03 * peak_value * (0.03 * peak_value)
epsilon = 1e-06
reach = 5
edge = 8
lanes = 128
half = 64
exact = lax.Precision.HIGHEST
windows = (5, 7, 11)


def vmem(limit):
    return pltpu.CompilerParams(vmem_limit_bytes=limit * 1024 * 1024)


def cost(seconds):
    return pl.CostEstimate(flops=int(seconds * 2e12), bytes_accessed=0, transcendentals=0)


def slab_sums(core, z_factor, offsets, me, slots, came=None):
    depth, rows, across = core.shape
    steps = 2
    block = rows // steps
    count = len(slots)

    def kernel(off, who, *refs):
        z_refs, core_ref, scale = refs[:count], refs[count], refs[-1]
        outs = refs[count + 1 : -1]
        if came is not None:
            came_ref, outs = outs[0], outs[1:]

        @pl.when(pl.program_id(0) == 0)
        def _():
            lane = lax.broadcasted_iota(jnp.int32, (depth, lanes), 1)
            for index, slot in enumerate(slots):
                at = off[who[0] ^ slot] % lanes
                column = jnp.sum(
                    jnp.where(lane == at, z_refs[index][...], 0.0), axis=1, keepdims=True
                )
                for k in range(depth):
                    scale[index, k] = jnp.broadcast_to(column[k : k + 1], (8, lanes))

        def step(t, _):
            base = pl.multiple_of(t * 16, 16)
            tiles = [
                (pl.ds(base + 8 * r, 8), slice(c * lanes, (c + 1) * lanes))
                for r in range(2)
                for c in range(across // lanes)
            ]
            held = [[core_ref[k, r, c] for r, c in tiles] for k in range(depth)]
            for index in range(count):
                if came is None:
                    sums = [None] * len(tiles)
                else:
                    sums = [came_ref[index, r, c] for r, c in tiles]
                for k in range(depth):
                    weight = scale[index, k]
                    for i in range(len(tiles)):
                        term = held[k][i] * weight
                        sums[i] = term if sums[i] is None else sums[i] + term
                for i, (r, c) in enumerate(tiles):
                    if came is None:
                        outs[0][index, r, c] = sums[i]
                    else:
                        outs[index][r, c] = sums[i]
            return 0

        lax.fori_loop(0, block // 16, step, 0)

    def z_spec(slot):
        return pl.BlockSpec((depth, lanes), lambda i, off, who: (0, off[who[0] ^ slot] // lanes))

    stack_spec = pl.BlockSpec((count, block, across), lambda i, off, who: (0, i, 0))
    if came is None:
        out_shape = jax.ShapeDtypeStruct((count, rows, across), jnp.float32)
        out_specs = stack_spec
    else:
        out_shape = [jax.ShapeDtypeStruct((rows, across), jnp.float32)] * count
        out_specs = [pl.BlockSpec((block, across), lambda i, off, who: (i, 0))] * count
    return pl.pallas_call(
        kernel,
        out_shape=out_shape,
        grid_spec=pltpu.PrefetchScalarGridSpec(
            num_scalar_prefetch=2,
            grid=(steps,),
            in_specs=[z_spec(s) for s in slots]
            + [pl.BlockSpec((depth, block, across), lambda i, off, who: (0, i, 0))]
            + ([] if came is None else [stack_spec]),
            out_specs=out_specs,
            scratch_shapes=[pltpu.VMEM((count, depth, 8, lanes), jnp.float32)],
        ),
        compiler_params=vmem(12),
        cost_estimate=cost(2e-6),
        name="slab_sums",
    )(offsets, me, *([z_factor] * count), core, *(() if came is None else (came,)))


def split_sums(parts, layer, layers, token):
    rows, across = parts[0].shape
    chunk = rows // layers

    def kernel(at, *refs):
        ins, outs = refs[: len(parts)], refs[len(parts) + 1 :]
        for m in range(layers):
            start = pl.multiple_of((at[0] ^ m) * chunk, chunk)
            total = ins[0][pl.ds(start, chunk), :]
            for other in ins[1:]:
                total = total + other[pl.ds(start, chunk), :]
            outs[m][...] = total

    return pl.pallas_call(
        kernel,
        out_shape=[jax.ShapeDtypeStruct((chunk, across), jnp.float32)] * layers,
        in_specs=[pl.BlockSpec(memory_space=pltpu.SMEM)]
        + [pl.BlockSpec(memory_space=pltpu.VMEM)] * len(parts)
        + [pl.BlockSpec(memory_space=pl.ANY)],
        compiler_params=vmem(4),
        name="split_sums",
    )(layer, *parts, token)


def expand_rows(chunks, layer, x_rows, planes, rows):
    layers = len(chunks)
    chunk, across = chunks[0].shape

    def kernel(at, *refs):
        pieces, x_ref, out, whole, product = refs[:layers], *refs[layers:]
        for m in range(layers):
            whole[pl.ds(pl.multiple_of((at[0] ^ m) * chunk, chunk), chunk), :] = pieces[m][...]
        product[...] = jnp.dot(
            x_ref[...], whole[...], precision=exact, preferred_element_type=jnp.float32
        )
        for q in range(planes):
            out[q] = product[q * rows : q * rows + rows + 2 * edge, :]

    return pl.pallas_call(
        kernel,
        out_shape=jax.ShapeDtypeStruct((planes, rows + 2 * edge, across), jnp.float32),
        in_specs=[pl.BlockSpec(memory_space=pltpu.SMEM)]
        + [pl.BlockSpec(memory_space=pltpu.VMEM)] * (layers + 1),
        scratch_shapes=[
            pltpu.VMEM((layers * chunk, across), jnp.float32),
            pltpu.VMEM((x_rows.shape[0], across), jnp.float32),
        ],
        compiler_params=vmem(6),
        name="expand_rows",
    )(layer, *chunks, x_rows)


def held_rows(rows):
    return -(-(rows + 2 * reach) // 4) * 4


def rebuild(block, y_padded, extended):
    planes, tall, depth = block.shape
    rows = tall - 2 * edge
    steps = 3
    wide = y_padded.shape[0] // steps
    held = held_rows(rows)

    def kernel(block_ref, y_ref, ext_ref, out, stats, left):
        @pl.when(pl.program_id(0) == 0)
        def _():
            for p in range(planes):
                left[:, p, :] = block_ref[p, edge - reach : edge - reach + held, :]
            stats[...] = jnp.zeros(stats.shape, jnp.float32)

        value = lax.dot_general(
            left[...].reshape(held * planes, depth),
            y_ref[...],
            (((1,), (1,)), ((), ())),
            precision=exact,
            preferred_element_type=jnp.float32,
        ).reshape(held, planes, wide)
        out[...] = value
        misfit = ext_ref[reach : reach + rows] - value[reach : reach + rows]
        squares = jnp.sum(misfit * misfit, axis=0)
        tops = jnp.max(jnp.abs(misfit), axis=0)
        square, top = stats[0], stats[1]
        for c in range(wide // lanes):
            square = square + squares[:, c * lanes : (c + 1) * lanes]
            top = jnp.maximum(top, tops[:, c * lanes : (c + 1) * lanes])
        stats[0] = square
        stats[1] = top

    strip = pl.BlockSpec((held, planes, wide), lambda i: (0, 0, i))
    return pl.pallas_call(
        kernel,
        grid=(steps,),
        out_shape=[
            jax.ShapeDtypeStruct(extended.shape, jnp.float32),
            jax.ShapeDtypeStruct((2, planes, lanes), jnp.float32),
        ],
        in_specs=[
            pl.BlockSpec(block.shape, lambda i: (0, 0, 0)),
            pl.BlockSpec((wide, depth), lambda i: (i, 0)),
            strip,
        ],
        out_specs=[
            strip,
            pl.BlockSpec((2, planes, lanes), lambda i: (0, 0, 0)),
        ],
        scratch_shapes=[pltpu.VMEM((held, planes, depth), jnp.float32)],
        compiler_params=vmem(18),
        cost_estimate=cost(6e-6),
        name="rebuild",
    )(block, y_padded, extended)


def down_sums(load, window, count):
    rows = [load(i) for i in range(count + window - 1)]
    pair = [rows[i] + rows[i + 1] for i in range(count + window - 2)]
    if window == 5:
        return [(pair[i] + pair[i + 2]) + rows[i + 4] for i in range(count)]
    if window == 7:
        return [(pair[i] + pair[i + 2]) + (pair[i + 4] + rows[i + 6]) for i in range(count)]
    four = [pair[i] + pair[i + 2] for i in range(count + 4)]
    return [(four[i] + four[i + 4]) + (pair[i + 8] + rows[i + 10]) for i in range(count)]


def band_matrix():
    source = lax.broadcasted_iota(jnp.int32, (2 * lanes, lanes), 0)
    target = lax.broadcasted_iota(jnp.int32, (2 * lanes, lanes), 1) + half
    apart = jnp.abs(source - target)
    return jnp.concatenate(
        [jnp.where(apart <= window // 2, 1.0, 0.0) for window in windows], axis=1
    ).astype(jnp.bfloat16)


def split_store(value, terms, field, at):
    for t in range(3):
        term = value.astype(jnp.bfloat16)
        terms[field, t, at, :] = term
        if t < 2:
            value = value - term.astype(jnp.float32)


def band_sums(band, terms, sums, f, c, held, planes):
    total = None
    for t in range(3):
        found = jnp.dot(
            terms[f, t, :, c * lanes : c * lanes + 2 * lanes],
            band,
            preferred_element_type=jnp.float32,
        )
        total = found if total is None else total + found
    for w in range(3):
        sums[f, w, c] = total[:, w * lanes : (w + 1) * lanes].reshape(held, planes, lanes)


def target_sums(initial, low, high, gate):
    rows, planes, across = initial.shape
    held = held_rows(rows)
    wide = 512
    steps = across // wide
    padded = across + 2 * lanes
    group = 8 if rows % 8 == 0 else 4

    def kernel(init_ref, low_ref, high_ref, gate_ref, ext, token, *refs):
        outs, (terms, sums) = refs[:3], refs[3:]
        step = pl.program_id(0)

        @pl.when(step == 0)
        def _():
            token[...] = jnp.zeros(token.shape, jnp.float32)

            def copy_row(ref):
                def go(x, at):
                    ext[at + x, :, 0:lanes] = jnp.zeros((planes, lanes), jnp.float32)
                    ext[at + x, :, across : across + 2 * lanes] = jnp.zeros(
                        (planes, 2 * lanes), jnp.float32
                    )
                    ext[at + x, :, half : half + across] = ref[x]
                    return at

                return go

            lax.fori_loop(0, reach, copy_row(low_ref), 0)
            lax.fori_loop(0, rows, copy_row(init_ref), reach)
            lax.fori_loop(0, reach, copy_row(high_ref), reach + rows)
            for x in range(rows + 2 * reach, held):
                ext[x] = jnp.zeros((planes, padded), jnp.float32)

        start = pl.multiple_of(step * wide, lanes)

        def split_step(t, _):
            value = ext[pl.ds(t * 2, 2), :, pl.ds(start, wide + lanes)]
            at = pl.ds(pl.multiple_of(t * 2 * planes, 2 * planes), 2 * planes)
            split_store(value.reshape(2 * planes, wide + lanes), terms, 0, at)
            return 0

        lax.fori_loop(0, held // 2, split_step, 0)
        band = band_matrix()

        def finish(c, base):
            part = slice(c * lanes, (c + 1) * lanes)
            for w, window in enumerate(windows):
                skip = reach - window // 2
                found = down_sums(lambda i: sums[0, w, c, base + skip + i], window, group)
                for i in range(group):
                    outs[w][base + i, :, part] = found[i] * (2.0 / (window * window))

        for c in range(wide // lanes + 1):
            if c < wide // lanes:
                band_sums(band, terms, sums, 0, c, held, planes)
            if c > 0:
                for t in range(rows // group):
                    finish(c - 1, t * group)

    some = pl.BlockSpec((reach, planes, across), lambda i: (0, 0, 0))
    out_spec = pl.BlockSpec((rows, planes, wide), lambda i: (0, 0, i))
    return pl.pallas_call(
        kernel,
        grid=(steps,),
        out_shape=[
            jax.ShapeDtypeStruct((held, planes, padded), jnp.float32),
            jax.ShapeDtypeStruct((8, lanes), jnp.float32),
        ]
        + [jax.ShapeDtypeStruct((rows, planes, across), jnp.float32)] * 3,
        in_specs=[
            pl.BlockSpec((rows, planes, across), lambda i: (0, 0, 0)),
            some,
            some,
            pl.BlockSpec(memory_space=pl.ANY),
        ],
        out_specs=[
            pl.BlockSpec((held, planes, padded), lambda i: (0, 0, 0)),
            pl.BlockSpec((8, lanes), lambda i: (0, 0)),
        ]
        + [out_spec] * 3,
        scratch_shapes=[
            pltpu.VMEM((1, 3, held * planes, wide + lanes), jnp.bfloat16),
            pltpu.VMEM((1, 3, wide // lanes, held, planes, lanes), jnp.float32),
        ],
        compiler_params=vmem(34),
        cost_estimate=cost(12e-6),
        name="target_sums",
    )(initial, low, high, gate)


def maps(extended, rebuilt, target, rows):
    held, planes, padded = extended.shape
    across = padded - 2 * lanes
    wide = 512
    steps = across // wide
    group = 8 if rows % 8 == 0 else 4
    fields = 3

    def kernel(ext_ref, reb_ref, *refs):
        target_refs, outs, (terms, sums) = refs[:3], refs[3:6], refs[6:]

        def split_step(t, _):
            a = ext_ref[pl.ds(t * 2, 2)].reshape(2 * planes, wide + lanes)
            b = reb_ref[pl.ds(t * 2, 2)].reshape(2 * planes, wide + lanes)
            product = a * b
            at = pl.ds(pl.multiple_of(t * 2 * planes, 2 * planes), 2 * planes)
            split_store(b, terms, 0, at)
            split_store(a * a + b * b, terms, 1, at)
            split_store(product + product, terms, 2, at)
            return 0

        lax.fori_loop(0, held // 2, split_step, 0)
        band = band_matrix()

        def finish(c, base):
            part = slice(c * lanes, (c + 1) * lanes)
            for w, window in enumerate(windows):
                area = float(window * window)
                skip = reach - window // 2
                found = [
                    down_sums(lambda i, f=f: sums[f, w, c, base + skip + i], window, group)
                    for f in range(fields)
                ]
                for i in range(group):
                    one, squares, double = (found[f][i] for f in range(fields))
                    other = target_refs[w][base + i, :, part]
                    twice = other * one
                    both = (other * other) * (0.25 * area) + (one * one) * (1.0 / area)
                    first = both + area * first_const
                    upper = (twice + area * first_const) * ((double - twice) + area * second_const)
                    lower = first * ((squares - both) + area * second_const)
                    outs[w][base + i, :, part] = upper / lower

        turns = rows // group
        for c in range(wide // lanes + 1):
            for f in range(fields):
                if c < wide // lanes:
                    band_sums(band, terms, sums, f, c, held, planes)
                if c > 0:
                    for t in range(turns * f // fields, turns * (f + 1) // fields):
                        finish(c - 1, t * group)

    out_spec = pl.BlockSpec((rows, planes, wide), lambda i: (0, 0, i))
    strip = pl.BlockSpec(
        (pl.Element(held), pl.Element(planes), pl.Element(wide + lanes)),
        lambda i: (0, 0, pl.multiple_of(i * wide, lanes)),
    )
    return pl.pallas_call(
        kernel,
        grid=(steps,),
        out_shape=[jax.ShapeDtypeStruct((rows, planes, across), jnp.float32)] * 3,
        in_specs=[strip, strip] + [out_spec] * 3,
        out_specs=[out_spec] * 3,
        scratch_shapes=[
            pltpu.VMEM((fields, 3, held * planes, wide + lanes), jnp.bfloat16),
            pltpu.VMEM((fields, 3, wide // lanes, held, planes, lanes), jnp.float32),
        ],
        compiler_params=vmem(38),
        cost_estimate=cost(25e-6),
        name="maps",
    )(extended, rebuilt, *target)


def body(count, core, x_factor, y_factor, z_factor, offsets, initial):
    planes = offsets.shape[0]
    rows = initial.shape[0]
    layers = count // planes
    across = y_factor.shape[0]
    index = lax.axis_index("rank").astype(jnp.int32)
    me = (index % planes).reshape(1)
    layer = (index // planes).reshape(1)

    def swap(value, mask):
        return lax.ppermute(value, "rank", [(i, i ^ mask) for i in range(count)])

    up = [(i, i + 1) for i in range(count - 1)]
    down = [(j, i) for i, j in up]
    low = lax.ppermute(initial[rows - reach :], "rank", up)
    high = lax.ppermute(initial[:reach], "rank", down)

    away = slab_sums(core, z_factor, offsets, me, tuple(range(1, planes, 2)))
    came = swap(away, 1)
    slots = slab_sums(core, z_factor, offsets, me, tuple(range(0, planes, 2)), came)
    parts = [slots[0]] + [swap(slots[i], 2 * i) for i in range(1, planes // 2)]
    extended, token, *target = target_sums(initial, low, high, slots[0])
    chunks = split_sums(parts, layer, layers, token)
    mine = chunks[0]
    for m in range(1, layers):
        mine = mine + swap(chunks[m], planes * m)
    pieces = [mine] + [swap(mine, planes * m) for m in range(1, layers)]
    padded = jnp.pad(x_factor, ((edge, edge), (0, 0)))
    x_rows = lax.dynamic_slice_in_dim(
        padded, layer[0] * (planes * rows), planes * rows + 2 * edge, axis=0
    )
    y_padded = jnp.pad(y_factor, ((half, 2 * lanes - half), (0, 0)))
    spread = expand_rows(pieces, layer, x_rows, planes, rows)
    groups = [[g * planes + q for q in range(planes)] for g in range(layers)]
    block = lax.all_to_all(
        spread, "rank", split_axis=0, concat_axis=0, tiled=True, axis_index_groups=groups
    )
    rebuilt, stats = rebuild(block, y_padded, extended)
    five, seven, eleven = maps(extended, rebuilt, target, rows)
    mask = 1
    while mask < count:
        other = swap(stats, mask)
        stats = jnp.stack((stats[0] + other[0], jnp.maximum(stats[1], other[1])))
        mask *= 2
    max_error = jnp.max(stats[1]).reshape(1)
    mean_square = jnp.sum(stats[0], axis=1) / float(x_factor.shape[0] * across)
    psnr = 10.0 * jnp.log10(peak_value * peak_value / (mean_square + epsilon))
    return max_error, psnr, five, seven, eleven


def solution(mesh):
    placed = (
        P("rank", "groups", None),
        P("groups", None),
        P("groups", None),
        P("rank", "groups"),
        P("groups"),
        P("rank", "groups", None),
    )
    return jax.shard_map(
        functools.partial(body, mesh.shape["rank"]),
        mesh=mesh,
        in_specs=placed,
        out_specs=(
            P("groups"),
            P("groups"),
            P("rank", "groups", None),
            P("rank", "groups", None),
            P("rank", "groups", None),
        ),
        check_vma=False,
    )
```

```python
import functools

import jax
import jax.numpy as jnp
from jax import lax
from jax.experimental import pallas as pl
from jax.experimental.pallas import tpu as pltpu
from jax.sharding import PartitionSpec as P

peak_value = 64.0
first_const = 0.01 * peak_value * (0.01 * peak_value)
second_const = 0.03 * peak_value * (0.03 * peak_value)
epsilon = 1e-06
reach = 5
edge = 8
lanes = 128
half = 64
exact = lax.Precision.HIGHEST
windows = (5, 7, 11)


def vmem(limit):
    return pltpu.CompilerParams(vmem_limit_bytes=limit * 1024 * 1024)


def cost(seconds):
    return pl.CostEstimate(flops=int(seconds * 2e12), bytes_accessed=0, transcendentals=0)


def slab_sums(core, z_factor, offsets, me, slots, came=None):
    depth, rows, across = core.shape
    steps = 2
    block = rows // steps
    count = len(slots)

    def kernel(off, who, *refs):
        z_refs, core_ref, scale = refs[:count], refs[count], refs[-1]
        outs = refs[count + 1 : -1]
        if came is not None:
            came_ref, outs = outs[0], outs[1:]

        @pl.when(pl.program_id(0) == 0)
        def _():
            lane = lax.broadcasted_iota(jnp.int32, (depth, lanes), 1)
            for index, slot in enumerate(slots):
                at = off[who[0] ^ slot] % lanes
                column = jnp.sum(
                    jnp.where(lane == at, z_refs[index][...], 0.0), axis=1, keepdims=True
                )
                for k in range(depth):
                    scale[index, k] = jnp.broadcast_to(column[k : k + 1], (8, lanes))

        def step(t, _):
            base = pl.multiple_of(t * 16, 16)
            tiles = [
                (pl.ds(base + 8 * r, 8), slice(c * lanes, (c + 1) * lanes))
                for r in range(2)
                for c in range(across // lanes)
            ]
            held = [[core_ref[k, r, c] for r, c in tiles] for k in range(depth)]
            for index in range(count):
                if came is None:
                    sums = [None] * len(tiles)
                else:
                    sums = [came_ref[index, r, c] for r, c in tiles]
                for k in range(depth):
                    weight = scale[index, k]
                    for i in range(len(tiles)):
                        term = held[k][i] * weight
                        sums[i] = term if sums[i] is None else sums[i] + term
                for i, (r, c) in enumerate(tiles):
                    if came is None:
                        outs[0][index, r, c] = sums[i]
                    else:
                        outs[index][r, c] = sums[i]
            return 0

        lax.fori_loop(0, block // 16, step, 0)

    def z_spec(slot):
        return pl.BlockSpec((depth, lanes), lambda i, off, who: (0, off[who[0] ^ slot] // lanes))

    stack_spec = pl.BlockSpec((count, block, across), lambda i, off, who: (0, i, 0))
    if came is None:
        out_shape = jax.ShapeDtypeStruct((count, rows, across), jnp.float32)
        out_specs = stack_spec
    else:
        out_shape = [jax.ShapeDtypeStruct((rows, across), jnp.float32)] * count
        out_specs = [pl.BlockSpec((block, across), lambda i, off, who: (i, 0))] * count
    return pl.pallas_call(
        kernel,
        out_shape=out_shape,
        grid_spec=pltpu.PrefetchScalarGridSpec(
            num_scalar_prefetch=2,
            grid=(steps,),
            in_specs=[z_spec(s) for s in slots]
            + [pl.BlockSpec((depth, block, across), lambda i, off, who: (0, i, 0))]
            + ([] if came is None else [stack_spec]),
            out_specs=out_specs,
            scratch_shapes=[pltpu.VMEM((count, depth, 8, lanes), jnp.float32)],
        ),
        compiler_params=vmem(12),
        cost_estimate=cost(2e-6),
        name="slab_sums",
    )(offsets, me, *([z_factor] * count), core, *(() if came is None else (came,)))


def split_sums(parts, layer, layers, token):
    rows, across = parts[0].shape
    chunk = rows // layers

    def kernel(at, *refs):
        ins, outs = refs[: len(parts)], refs[len(parts) + 1 :]
        for m in range(layers):
            start = pl.multiple_of((at[0] ^ m) * chunk, chunk)
            total = ins[0][pl.ds(start, chunk), :]
            for other in ins[1:]:
                total = total + other[pl.ds(start, chunk), :]
            outs[m][...] = total

    return pl.pallas_call(
        kernel,
        out_shape=[jax.ShapeDtypeStruct((chunk, across), jnp.float32)] * layers,
        in_specs=[pl.BlockSpec(memory_space=pltpu.SMEM)]
        + [pl.BlockSpec(memory_space=pltpu.VMEM)] * len(parts)
        + [pl.BlockSpec(memory_space=pl.ANY)],
        compiler_params=vmem(4),
        name="split_sums",
    )(layer, *parts, token)


def expand_rows(chunks, layer, x_rows, planes, rows, gate):
    layers = len(chunks)
    chunk, across = chunks[0].shape

    def kernel(at, *refs):
        pieces, x_ref, _, out, whole, product = refs[:layers], *refs[layers:]
        for m in range(layers):
            whole[pl.ds(pl.multiple_of((at[0] ^ m) * chunk, chunk), chunk), :] = pieces[m][...]
        product[...] = jnp.dot(
            x_ref[...], whole[...], precision=exact, preferred_element_type=jnp.float32
        )
        for q in range(planes):
            out[q] = product[q * rows : q * rows + rows + 2 * edge, :]

    return pl.pallas_call(
        kernel,
        out_shape=jax.ShapeDtypeStruct((planes, rows + 2 * edge, across), jnp.float32),
        in_specs=[pl.BlockSpec(memory_space=pltpu.SMEM)]
        + [pl.BlockSpec(memory_space=pltpu.VMEM)] * (layers + 1)
        + [pl.BlockSpec(memory_space=pl.ANY)],
        scratch_shapes=[
            pltpu.VMEM((layers * chunk, across), jnp.float32),
            pltpu.VMEM((x_rows.shape[0], across), jnp.float32),
        ],
        compiler_params=vmem(6),
        name="expand_rows",
    )(layer, *chunks, x_rows, gate)


def held_rows(rows):
    return -(-(rows + 2 * reach) // 4) * 4


def rebuild(block, y_padded, extended):
    planes, tall, depth = block.shape
    rows = tall - 2 * edge
    steps = 6
    wide = y_padded.shape[0] // steps
    held = held_rows(rows)

    def kernel(block_ref, y_ref, ext_ref, out, stats, left):
        @pl.when(pl.program_id(0) == 0)
        def _():
            for p in range(planes):
                left[:, p, :] = block_ref[p, edge - reach : edge - reach + held, :]
            stats[...] = jnp.zeros(stats.shape, jnp.float32)

        value = lax.dot_general(
            left[...].reshape(held * planes, depth),
            y_ref[...],
            (((1,), (1,)), ((), ())),
            precision=exact,
            preferred_element_type=jnp.float32,
        ).reshape(held, planes, wide)
        out[...] = value
        misfit = ext_ref[reach : reach + rows] - value[reach : reach + rows]
        squares = jnp.sum(misfit * misfit, axis=0)
        tops = jnp.max(jnp.abs(misfit), axis=0)
        square, top = stats[0], stats[1]
        for c in range(wide // lanes):
            square = square + squares[:, c * lanes : (c + 1) * lanes]
            top = jnp.maximum(top, tops[:, c * lanes : (c + 1) * lanes])
        stats[0] = square
        stats[1] = top

    strip = pl.BlockSpec((held, planes, wide), lambda i: (0, 0, i))
    return pl.pallas_call(
        kernel,
        grid=(steps,),
        out_shape=[
            jax.ShapeDtypeStruct(extended.shape, jnp.float32),
            jax.ShapeDtypeStruct((2, planes, lanes), jnp.float32),
        ],
        in_specs=[
            pl.BlockSpec(block.shape, lambda i: (0, 0, 0)),
            pl.BlockSpec((wide, depth), lambda i: (i, 0)),
            strip,
        ],
        out_specs=[
            strip,
            pl.BlockSpec((2, planes, lanes), lambda i: (0, 0, 0)),
        ],
        scratch_shapes=[pltpu.VMEM((held, planes, depth), jnp.float32)],
        compiler_params=vmem(60),
        cost_estimate=cost(6e-6),
        name="rebuild",
    )(block, y_padded, extended)


def down_sums(load, window, count):
    rows = [load(i) for i in range(count + window - 1)]
    pair = [rows[i] + rows[i + 1] for i in range(count + window - 2)]
    if window == 5:
        return [(pair[i] + pair[i + 2]) + rows[i + 4] for i in range(count)]
    if window == 7:
        return [(pair[i] + pair[i + 2]) + (pair[i + 4] + rows[i + 6]) for i in range(count)]
    four = [pair[i] + pair[i + 2] for i in range(count + 4)]
    return [(four[i] + four[i + 4]) + (pair[i + 8] + rows[i + 10]) for i in range(count)]


def band_matrix():
    source = lax.broadcasted_iota(jnp.int32, (2 * lanes, lanes), 0)
    target = lax.broadcasted_iota(jnp.int32, (2 * lanes, lanes), 1) + half
    apart = jnp.abs(source - target)
    return jnp.concatenate(
        [jnp.where(apart <= window // 2, 1.0, 0.0) for window in windows], axis=1
    ).astype(jnp.bfloat16)


def split_store(value, terms, field, at):
    for t in range(3):
        term = value.astype(jnp.bfloat16)
        terms[field, t, at, :] = term
        if t < 2:
            value = value - term.astype(jnp.float32)


def band_sums(band, terms, sums, f, c, held, planes):
    total = None
    for t in range(3):
        found = jnp.dot(
            terms[f, t, :, c * lanes : c * lanes + 2 * lanes],
            band,
            preferred_element_type=jnp.float32,
        )
        total = found if total is None else total + found
    for w in range(3):
        sums[f, w, c] = total[:, w * lanes : (w + 1) * lanes].reshape(held, planes, lanes)


def target_block(strip_of, outs, terms, sums, held, planes, rows, wide):
    group = 8 if rows % 8 == 0 else 4

    def split_step(t, _):
        at = pl.ds(pl.multiple_of(t * 2 * planes, 2 * planes), 2 * planes)
        split_store(strip_of(t).reshape(2 * planes, wide + lanes), terms, 0, at)
        return 0

    lax.fori_loop(0, held // 2, split_step, 0)
    band = band_matrix()

    def finish(c, base):
        part = slice(c * lanes, (c + 1) * lanes)
        for w, window in enumerate(windows):
            skip = reach - window // 2
            found = down_sums(lambda i: sums[0, w, c, base + skip + i], window, group)
            for i in range(group):
                outs[w][base + i, :, part] = found[i] * (2.0 / (window * window))

    for c in range(wide // lanes + 1):
        if c < wide // lanes:
            band_sums(band, terms, sums, 0, c, held, planes)
        if c > 0:
            for t in range(rows // group):
                finish(c - 1, t * group)


def target_scratch(held, planes, wide):
    return [
        pltpu.VMEM((1, 3, held * planes, wide + lanes), jnp.bfloat16),
        pltpu.VMEM((1, 3, wide // lanes, held, planes, lanes), jnp.float32),
    ]


def target_first(initial, low, high, gate, wide, steps):
    rows, planes, across = initial.shape
    held = held_rows(rows)
    padded = across + 2 * lanes

    def kernel(init_ref, low_ref, high_ref, gate_ref, ext, token, *refs):
        outs, (terms, sums) = refs[:3], refs[3:]
        step = pl.program_id(0)

        @pl.when(step == 0)
        def _():
            token[...] = jnp.zeros(token.shape, jnp.float32)

            def copy_row(ref):
                def go(x, at):
                    ext[at + x, :, 0:lanes] = jnp.zeros((planes, lanes), jnp.float32)
                    ext[at + x, :, across : across + 2 * lanes] = jnp.zeros(
                        (planes, 2 * lanes), jnp.float32
                    )
                    ext[at + x, :, half : half + across] = ref[x]
                    return at

                return go

            lax.fori_loop(0, reach, copy_row(low_ref), 0)
            lax.fori_loop(0, rows, copy_row(init_ref), reach)
            lax.fori_loop(0, reach, copy_row(high_ref), reach + rows)
            for x in range(rows + 2 * reach, held):
                ext[x] = jnp.zeros((planes, padded), jnp.float32)

        start = pl.multiple_of(step * wide, lanes)
        target_block(
            lambda t: ext[pl.ds(t * 2, 2), :, pl.ds(start, wide + lanes)],
            outs, terms, sums, held, planes, rows, wide,
        )

    some = pl.BlockSpec((reach, planes, across), lambda i: (0, 0, 0))
    return pl.pallas_call(
        kernel,
        grid=(steps,),
        out_shape=[
            jax.ShapeDtypeStruct((held, planes, padded), jnp.float32),
            jax.ShapeDtypeStruct((8, lanes), jnp.float32),
        ]
        + [jax.ShapeDtypeStruct((rows, planes, wide * steps), jnp.float32)] * 3,
        in_specs=[
            pl.BlockSpec((rows, planes, across), lambda i: (0, 0, 0)),
            some,
            some,
            pl.BlockSpec(memory_space=pl.ANY),
        ],
        out_specs=[
            pl.BlockSpec((held, planes, padded), lambda i: (0, 0, 0)),
            pl.BlockSpec((8, lanes), lambda i: (0, 0)),
        ]
        + [pl.BlockSpec((rows, planes, wide), lambda i: (0, 0, i))] * 3,
        scratch_shapes=target_scratch(held, planes, wide),
        compiler_params=vmem(60),
        cost_estimate=cost(9e-6),
        name="target_first",
    )(initial, low, high, gate)


def strips(held, planes, wide, first):
    return pl.BlockSpec(
        (pl.Element(held), pl.Element(planes), pl.Element(wide + lanes)),
        lambda i: (0, 0, pl.multiple_of((i + first) * wide, lanes)),
    )


def target_rest(extended, gate, rows, wide, first, steps):
    held, planes, _ = extended.shape

    def kernel(ext_ref, gate_ref, token, *refs):
        outs, (terms, sums) = refs[:3], refs[3:]
        token[...] = jnp.zeros(token.shape, jnp.float32)
        target_block(
            lambda t: ext_ref[pl.ds(t * 2, 2)], outs, terms, sums, held, planes, rows, wide
        )

    return pl.pallas_call(
        kernel,
        grid=(steps,),
        out_shape=[jax.ShapeDtypeStruct((8, lanes), jnp.float32)]
        + [jax.ShapeDtypeStruct((rows, planes, wide * steps), jnp.float32)] * 3,
        in_specs=[strips(held, planes, wide, first), pl.BlockSpec(memory_space=pl.ANY)],
        out_specs=[pl.BlockSpec((8, lanes), lambda i: (0, 0))]
        + [pl.BlockSpec((rows, planes, wide), lambda i: (0, 0, i))] * 3,
        scratch_shapes=target_scratch(held, planes, wide),
        compiler_params=vmem(60),
        cost_estimate=cost(7e-6),
        name="target_rest",
    )(extended, gate)


def maps(extended, rebuilt, early, late, rows, wide):
    held, planes, padded = extended.shape
    across = padded - 2 * lanes
    steps = across // wide
    turn = early[0].shape[2] // wide
    group = 8 if rows % 8 == 0 else 4
    fields = 3

    def kernel(ext_ref, reb_ref, *refs):
        early_refs, late_refs, outs, (terms, sums) = refs[:3], refs[3:6], refs[6:9], refs[9:]
        is_early = pl.program_id(0) < turn

        def split_step(t, _):
            a = ext_ref[pl.ds(t * 2, 2)].reshape(2 * planes, wide + lanes)
            b = reb_ref[pl.ds(t * 2, 2)].reshape(2 * planes, wide + lanes)
            product = a * b
            at = pl.ds(pl.multiple_of(t * 2 * planes, 2 * planes), 2 * planes)
            split_store(b, terms, 0, at)
            split_store(a * a + b * b, terms, 1, at)
            split_store(product + product, terms, 2, at)
            return 0

        lax.fori_loop(0, held // 2, split_step, 0)
        band = band_matrix()

        def finish(c, base):
            part = slice(c * lanes, (c + 1) * lanes)
            for w, window in enumerate(windows):
                area = float(window * window)
                skip = reach - window // 2
                found = [
                    down_sums(lambda i, f=f: sums[f, w, c, base + skip + i], window, group)
                    for f in range(fields)
                ]
                for i in range(group):
                    one, squares, double = (found[f][i] for f in range(fields))
                    other = jnp.where(
                        is_early, early_refs[w][base + i, :, part], late_refs[w][base + i, :, part]
                    )
                    twice = other * one
                    both = (other * other) * (0.25 * area) + (one * one) * (1.0 / area)
                    first = both + area * first_const
                    upper = (twice + area * first_const) * ((double - twice) + area * second_const)
                    lower = first * ((squares - both) + area * second_const)
                    outs[w][base + i, :, part] = upper / lower

        turns = rows // group
        for c in range(wide // lanes + 1):
            for f in range(fields):
                if c < wide // lanes:
                    band_sums(band, terms, sums, f, c, held, planes)
                if c > 0:
                    for t in range(turns * f // fields, turns * (f + 1) // fields):
                        finish(c - 1, t * group)

    out_spec = pl.BlockSpec((rows, planes, wide), lambda i: (0, 0, i))
    strip = strips(held, planes, wide, 0)
    early_spec = pl.BlockSpec((rows, planes, wide), lambda i: (0, 0, jnp.minimum(i, turn - 1)))
    late_spec = pl.BlockSpec((rows, planes, wide), lambda i: (0, 0, jnp.maximum(i - turn, 0)))
    return pl.pallas_call(
        kernel,
        grid=(steps,),
        out_shape=[jax.ShapeDtypeStruct((rows, planes, across), jnp.float32)] * 3,
        in_specs=[strip, strip] + [early_spec] * 3 + [late_spec] * 3,
        out_specs=[out_spec] * 3,
        scratch_shapes=[
            pltpu.VMEM((fields, 3, held * planes, wide + lanes), jnp.bfloat16),
            pltpu.VMEM((fields, 3, wide // lanes, held, planes, lanes), jnp.float32),
        ],
        compiler_params=vmem(60),
        cost_estimate=cost(25e-6),
        name="maps",
    )(extended, rebuilt, *early, *late)


def body(count, core, x_factor, y_factor, z_factor, offsets, initial):
    planes = offsets.shape[0]
    rows = initial.shape[0]
    layers = count // planes
    across = y_factor.shape[0]
    index = lax.axis_index("rank").astype(jnp.int32)
    me = (index % planes).reshape(1)
    layer = (index // planes).reshape(1)

    def swap(value, mask):
        return lax.ppermute(value, "rank", [(i, i ^ mask) for i in range(count)])

    up = [(i, i + 1) for i in range(count - 1)]
    down = [(j, i) for i, j in up]
    low = lax.ppermute(initial[rows - reach :], "rank", up)
    high = lax.ppermute(initial[:reach], "rank", down)

    away = slab_sums(core, z_factor, offsets, me, tuple(range(1, planes, 2)))
    came = swap(away, 1)
    slots = slab_sums(core, z_factor, offsets, me, tuple(range(0, planes, 2)), came)
    parts = [slots[0]] + [swap(slots[i], 2 * i) for i in range(1, planes // 2)]
    wide = 4 * lanes
    turn = across // wide // 2
    extended, token, *early = target_first(initial, low, high, slots[0], wide, turn)
    chunks = split_sums(parts, layer, layers, token)
    mine = chunks[0]
    for m in range(1, layers):
        mine = mine + swap(chunks[m], planes * m)
    pieces = [mine] + [swap(mine, planes * m) for m in range(1, layers)]
    token, *late = target_rest(extended, mine, rows, wide, turn, across // wide - turn)
    padded = jnp.pad(x_factor, ((edge, edge), (0, 0)))
    x_rows = lax.dynamic_slice_in_dim(
        padded, layer[0] * (planes * rows), planes * rows + 2 * edge, axis=0
    )
    y_padded = jnp.pad(y_factor, ((half, 2 * lanes - half), (0, 0)))
    spread = expand_rows(pieces, layer, x_rows, planes, rows, token)
    groups = [[g * planes + q for q in range(planes)] for g in range(layers)]
    block = lax.all_to_all(
        spread, "rank", split_axis=0, concat_axis=0, tiled=True, axis_index_groups=groups
    )
    rebuilt, stats = rebuild(block, y_padded, extended)
    five, seven, eleven = maps(extended, rebuilt, early, late, rows, wide)
    mask = 1
    while mask < count:
        other = swap(stats, mask)
        stats = jnp.stack((stats[0] + other[0], jnp.maximum(stats[1], other[1])))
        mask *= 2
    max_error = jnp.max(stats[1]).reshape(1)
    mean_square = jnp.sum(stats[0], axis=1) / float(x_factor.shape[0] * across)
    psnr = 10.0 * jnp.log10(peak_value * peak_value / (mean_square + epsilon))
    return max_error, psnr, five, seven, eleven


def solution(mesh):
    placed = (
        P("rank", "groups", None),
        P("groups", None),
        P("groups", None),
        P("rank", "groups"),
        P("groups"),
        P("rank", "groups", None),
    )
    return jax.shard_map(
        functools.partial(body, mesh.shape["rank"]),
        mesh=mesh,
        in_specs=placed,
        out_specs=(
            P("groups"),
            P("groups"),
            P("rank", "groups", None),
            P("rank", "groups", None),
            P("rank", "groups", None),
        ),
        check_vma=False,
    )
```
